32 devices in a mesh: gx: 8 (over z, y), gy: 4 (over x, core).
Axes of the slice: x: 2, y: 2, z: 4, core: 2. Of those that a mesh axis runs over, the one named last changes fastest.
Arguments:
- modes: float32 [16, 3, 32, 32, 128], P(None, None, 'gx', 'gy'), may hold values from -0.03 to 0.03
- region: int32 [32, 32, 128], P('gx', 'gy'), may hold values from 0 to 15
- stiffness: float32 [16], replicated, may hold values from 0.1 to 10
- coarse_group: int32 [8, 4], replicated, may hold values from 0 to 3
Outputs:
- coarse: float32 [8, 64, 192], P('gx', 'gy')
The draws below stay inside these ranges and needn't reach their ends.
All inputs are finite; a program needn't handle non-finite values.
Results may differ from the reference program's by a relative error of at most 0.0003.
Values sent between devices are 32-bit elements; how exact they have to be, the bound alone decides.
A program may use at most 128 MiB of HBM per device.

```python
import math
import jax
import jax.numpy as jnp
from jax import lax

MODES = 16
GROUPS = 4
REGIONS = 16
CX = 4
CY = 8
NZ = 128
NX = 32
NY = 32
N_GX = 8
N_GY = 4


def draw_modes(key, part):
    sigma = 0.0015
    wave_count = 4
    key_rough = jax.random.fold_in(key, 11)
    key_wave = jax.random.fold_in(key, 12)
    two_pi = 2.0 * math.pi
    freq_x = jax.random.uniform(jax.random.fold_in(key_wave, 1), (MODES, 3, wave_count), jnp.float32, 0.15, 0.6) * (two_pi / CX)
    freq_y = jax.random.uniform(jax.random.fold_in(key_wave, 2), (MODES, 3, wave_count), jnp.float32, 0.15, 0.6) * (two_pi / CY)
    freq_z = jax.random.uniform(jax.random.fold_in(key_wave, 3), (MODES, 3, wave_count), jnp.float32, 0.15, 0.6) * (two_pi / 16.0)
    sign_x = jax.random.rademacher(jax.random.fold_in(key_wave, 4), (MODES, 3, wave_count), jnp.float32)
    sign_y = jax.random.rademacher(jax.random.fold_in(key_wave, 5), (MODES, 3, wave_count), jnp.float32)
    phases = jax.random.uniform(jax.random.fold_in(key_wave, 6), (MODES, 3, wave_count), jnp.float32, 0.0, two_pi)
    freq_x = freq_x * sign_x
    freq_y = freq_y * sign_y
    amplitude = sigma / math.sqrt(0.5 * wave_count)
    coord_x = jnp.arange(NX, dtype=jnp.float32)[:, None, None]
    coord_y = jnp.arange(NY, dtype=jnp.float32)[None, :, None]
    coord_z = jnp.arange(NZ, dtype=jnp.float32)[None, None, :]

    def one_mode(index):
        key_mode = jax.random.fold_in(key_rough, index)
        noise = jax.random.truncated_normal(key_mode, -4.0, 4.0, (3, NX, NY, NZ), jnp.float32)
        for axis_num in (1, 2, 3):
            noise = noise + 0.6 * (jnp.roll(noise, 1, axis_num) + jnp.roll(noise, -1, axis_num))
        rough = noise * (sigma / 1.72 ** 1.5)
        mode_fx = freq_x[index]
        mode_fy = freq_y[index]
        mode_fz = freq_z[index]
        mode_phase = phases[index]
        comps = []
        for comp in range(3):
            total = jnp.zeros((NX, NY, NZ), jnp.float32)
            for wave in range(wave_count):
                angle_now = mode_fx[comp, wave] * coord_x + mode_fy[comp, wave] * coord_y + mode_fz[comp, wave] * coord_z + mode_phase[comp, wave]
                total = total + amplitude * jnp.cos(angle_now)
            comps.append(total)
        return rough + jnp.stack(comps)
    fields = lax.map(one_mode, jnp.arange(MODES, dtype=jnp.int32))
    return jnp.clip(fields, -0.029, 0.029)


def plant(entries, own_key, smallest, high):
    dims = entries.shape
    index_at = [jax.random.randint(jax.random.fold_in(own_key, axis), (), 0, dims[axis]) for axis in range(len(dims))]
    entries = entries.at[tuple(index_at)].set(smallest)
    longest = dims.index(max(dims))
    index_at[longest] = (index_at[longest] + 1) % dims[longest]
    return entries.at[tuple(index_at)].set(high)


def setup_inputs(seed: int = 0) -> dict:
    streams_of = jax.random.split(jax.random.key(seed), 5)
    modes = draw_modes(jax.random.fold_in(streams_of[4], 71), 0)
    region = plant(jax.random.randint(streams_of[1], (NX, NY, NZ), 0, REGIONS), jax.random.fold_in(streams_of[1], 1), 0, REGIONS - 1).astype(jnp.int32)
    stiffness = jnp.clip(jnp.exp(jax.random.uniform(streams_of[2], (REGIONS,), jnp.float32, math.log(0.1), math.log(10.0))), 0.1, 10.0)
    coarse_group = plant(jax.random.randint(streams_of[3], (N_GX, N_GY), 0, GROUPS), jax.random.fold_in(streams_of[3], 1), 0, GROUPS - 1).astype(jnp.int32)
    return dict(modes=modes, region=region, stiffness=stiffness, coarse_group=coarse_group)


beta_shear = 0.5
mass_share = 0.1


def all_offsets():
    return [(shift_x, shift_y, shift_z) for shift_x in (-1, 0, 1) for shift_y in (-1, 0, 1) for shift_z in (-1, 0, 1) if (shift_x, shift_y, shift_z) != (0, 0, 0)]


def apply_operator(padded, stiff_pad):
    span_x = padded.shape[2] - 2
    span_y = padded.shape[3] - 2
    span_z = padded.shape[4] - 2
    centre = padded[:, :, 1:span_x + 1, 1:span_y + 1, 1:span_z + 1]
    stiff_here = stiff_pad[1:span_x + 1, 1:span_y + 1, 1:span_z + 1]
    result = mass_share * stiff_here * centre
    for step_x, step_y, step_z in all_offsets():
        reach_len = abs(step_x) + abs(step_y) + abs(step_z)
        weight = 0.5 ** (reach_len - 1)
        nearby = padded[:, :, 1 + step_x:1 + step_x + span_x, 1 + step_y:1 + step_y + span_y, 1 + step_z:1 + step_z + span_z]
        stiff_there = stiff_pad[1 + step_x:1 + step_x + span_x, 1 + step_y:1 + step_y + span_y, 1 + step_z:1 + step_z + span_z]
        coupling = (0.5 * weight) * (stiff_here + stiff_there)
        differ = centre - nearby
        along_dir = (beta_shear / reach_len) * (step_x * differ[:, 0] + step_y * differ[:, 1] + step_z * differ[:, 2])
        pushed = differ + jnp.stack([step_x * along_dir, step_y * along_dir, step_z * along_dir], axis=1)
        result = result + coupling * pushed
    return result


def pair_blocks(applied, mode_cycle):
    span_x = mode_cycle.shape[2] - 2
    span_y = mode_cycle.shape[3] - 2
    bounds_x = [(0, 1), (1, span_x + 1), (span_x + 1, span_x + 2)]
    bounds_y = [(0, 1), (1, span_y + 1), (span_y + 1, span_y + 2)]
    rows_out = []
    for low_x, high_x in bounds_x:
        cols_out = []
        for low_y, high_y in bounds_y:
            cols_out.append(jnp.einsum('kaxyz,jaxyz->kj', applied[:, :, low_x:high_x, low_y:high_y], mode_cycle[:, :, low_x:high_x, low_y:high_y], precision=lax.Precision.HIGHEST))
        rows_out.append(jnp.stack(cols_out))
    return jnp.stack(rows_out)


def reference(modes, region, stiffness, coarse_group):
    stiff_cells = stiffness[region]
    cycle_pad = jnp.pad(modes, ((0, 0), (0, 0), (1, 1), (1, 1), (0, 0)))
    stiff_all = jnp.pad(stiff_cells, ((2, 2), (2, 2), (1, 1)))

    def one_block(sub_index):
        strip_row = (sub_index // N_GY).astype(jnp.int32)
        strip_col = (sub_index % N_GY).astype(jnp.int32)
        start_x = (strip_row * CX).astype(jnp.int32)
        start_y = (strip_col * CY).astype(jnp.int32)
        anchor = jnp.zeros((), jnp.int32)
        mode_cycle = lax.dynamic_slice(cycle_pad, (anchor, anchor, start_x, start_y, anchor), (MODES, 3, CX + 2, CY + 2, NZ))
        own_modes = lax.dynamic_slice(modes, (anchor, anchor, start_x, start_y, anchor), (MODES, 3, CX, CY, NZ))
        padded = jnp.pad(own_modes, ((0, 0), (0, 0), (2, 2), (2, 2), (1, 1)))
        stiff_pad = lax.dynamic_slice(stiff_all, (start_x, start_y, anchor), (CX + 4, CY + 4, NZ + 2))
        applied = apply_operator(padded, stiff_pad)
        return pair_blocks(applied, mode_cycle)

    blocks = lax.map(one_block, jnp.arange(N_GX * N_GY, dtype=jnp.int32))
    blocks = blocks.reshape(N_GX, N_GY, 3, 3, MODES, MODES)
    group_pad = jnp.pad(coarse_group, 1, constant_values=-1)
    near_groups = jnp.stack([jnp.stack([group_pad[1 + shift_x:1 + shift_x + N_GX, 1 + shift_y:1 + shift_y + N_GY] for shift_y in (-1, 0, 1)]) for shift_x in (-1, 0, 1)])
    labels = jnp.arange(GROUPS, dtype=jnp.int32)
    hot_near = (near_groups[..., None] == labels).astype(jnp.float32)
    hot_self = (coarse_group[..., None] == labels).astype(jnp.float32)
    coarse = jnp.einsum('abg,abxykj,xyabh->agkxhj', hot_self, blocks, hot_near, precision=lax.Precision.HIGHEST)
    return coarse.reshape(N_GX, GROUPS * MODES, 3 * GROUPS * MODES)
```

```python
import functools

import jax
import jax.numpy as jnp
from jax import lax
from jax.experimental import pallas as pl
from jax.experimental.pallas import tpu as pltpu
from jax.sharding import PartitionSpec as P

GROUPS = 4

beta_shear = 0.5
mass_share = 0.1

W1, W2, W3 = 0.5, 0.25, 0.125
B1, B2, B3 = W1 * beta_shear, W2 * beta_shear / 2, W3 * beta_shear / 3
DIAG_SUM = 6 * W1 + 12 * W2 + 8 * W3 + 2 * B1 + 8 * B2 + 8 * B3

MESH = pl.DeviceIdType.MESH
RING = [(-1, -1), (-1, 0), (-1, 1), (0, -1), (0, 1), (1, -1), (1, 0), (1, 1)]
HELD = [(1, 0), (0, 1), (1, -1), (1, 1)]


def lane_steps(value):
    lane = lax.broadcasted_iota(jnp.int32, value.shape, value.ndim - 1)
    size = value.shape[-1]
    before = jnp.where(lane == 0, 0.0, pltpu.roll(value, 1, value.ndim - 1))
    after = jnp.where(lane == size - 1, 0.0, pltpu.roll(value, size - 1, value.ndim - 1))
    return before + after, after - before


def plane_parts(fields, low, high):
    span = fields[0].shape[0]

    def at(value, step):
        first, last = low + step, high + step
        start, stop = min(max(first, 0), span), min(max(last, 0), span)
        zeros = lambda n: [jnp.zeros((n,) + value.shape[1:], value.dtype)] if n else []
        if start >= stop:
            return zeros(last - first)[0]
        pieces = zeros(start - first) + [value[start:stop]] + zeros(last - stop)
        return pieces[0] if len(pieces) == 1 else jnp.concatenate(pieces, axis=0)

    def even(value):
        return at(value, -1) + at(value, 1)

    def odd(value):
        return at(value, 1) - at(value, -1)

    vx, vy, vz = fields
    (ex, ox), (ey, oy), (ez, oz) = [lane_steps(v) for v in fields]
    level = at(W1 * ex, 0) + even(W1 * vx + W2 * ex)
    share = at((W1 + B1) * vx + (W2 + B2) * ex, 0) + even((W2 + B2) * vx + (W3 + B3) * ex)
    turn = odd(B2 * vy + B3 * ey) + B2 * at(oz, 0) + B3 * even(oz)
    out_x = (level, share + turn, share - turn)
    skew = odd(oz)
    level = at(W1 * ey, 0) + even((W1 + B1) * vy + (W2 + B2) * ey) + B2 * skew
    share = at(W1 * vy + W2 * ey, 0) + even((W2 + B2) * vy + (W3 + B3) * ey) + B3 * skew
    turn = odd(B2 * vx + B3 * ex)
    out_y = (level, share + turn, share - turn)
    skew = odd(oy)
    wide = W1 * vz + (W2 + B2) * ez
    level = at((W1 + B1) * ez, 0) + even(wide) + B2 * skew
    share = at(wide, 0) + even(W2 * vz + (W3 + B3) * ez) + B3 * skew
    turn = B2 * at(ox, 0) + B3 * even(ox)
    out_z = (level, share + turn, share - turn)
    here, before, after = zip(out_x, out_y, out_z)
    return here, before, after


def stacked(value):
    high = value.astype(jnp.bfloat16)
    low = (value - high.astype(jnp.float32)).astype(jnp.bfloat16)
    cells = value.shape[0]
    join = lambda part: jnp.concatenate([part[i] for i in range(cells)], axis=1)
    return jnp.concatenate([join(high), join(low)], axis=0)


def product(left, right):
    return lax.dot_general(
        left, right, (((1,), (1,)), ((), ())), preferred_element_type=jnp.float32
    )


def folded(value, width):
    value = value[:width] + value[width:]
    return value[:, :width] + value[:, width:]


def kernel(
    shape, counts, modes, region, stiff, group, out,
    field, cells, ring_row, ring_side, ring_corner, sigma, diag,
    halo_x, halo_y, halo_c, part_a, part_b, got_a, got_b,
    load_sem, ring_send, ring_recv, halo_send, halo_recv, a_send, a_recv, b_send, b_recv,
):
    width, span_x, span_y, span_z = shape
    count_x, count_y = counts
    rows = GROUPS * width // count_y
    me_x, me_y = lax.axis_index("gx"), lax.axis_index("gy")

    def exists(step_x, step_y):
        ok = me_x >= 0
        if step_x < 0:
            ok = jnp.logical_and(ok, me_x > 0)
        if step_x > 0:
            ok = jnp.logical_and(ok, me_x < count_x - 1)
        if step_y < 0:
            ok = jnp.logical_and(ok, me_y > 0)
        if step_y > 0:
            ok = jnp.logical_and(ok, me_y < count_y - 1)
        return ok

    def where_is(step_x, step_y):
        return {"gx": me_x + step_x, "gy": me_y + step_y}

    load_modes = pltpu.make_async_copy(modes, field, load_sem.at[0])
    load_region = pltpu.make_async_copy(region, cells, load_sem.at[1])
    load_region.start()
    load_modes.start()

    barrier = pltpu.get_barrier_semaphore()
    for step_x in (-1, 0, 1):
        @pl.when(exists(step_x, 0))
        def _():
            for other in range(1 if step_x == 0 else 0, count_y):
                there = lax.rem(me_y + other, count_y)
                pl.semaphore_signal(
                    barrier, inc=1,
                    device_id={"gx": me_x + step_x, "gy": there}, device_id_type=MESH,
                )
    strips = 1 + (me_x > 0).astype(jnp.int32) + (me_x < count_x - 1).astype(jnp.int32)
    pl.semaphore_wait(barrier, strips * count_y - 1)

    def ring_refs(slot):
        step_x, step_y = RING[slot]
        if step_x == 0:
            return region, ring_side.at[(step_y + 1) // 2]
        plane = region.at[0 if step_x > 0 else span_x - 1]
        if step_y == 0:
            return plane, ring_row.at[(step_x + 1) // 2]
        return plane, ring_corner.at[(step_x + 1) + (step_y + 1) // 2]

    def ring_copy(slot):
        step_x, step_y = RING[slot]
        source, target = ring_refs(slot)
        return pltpu.make_async_remote_copy(
            src_ref=source, dst_ref=target,
            send_sem=ring_send.at[slot], recv_sem=ring_recv.at[slot],
            device_id=where_is(-step_x, -step_y), device_id_type=MESH,
        )

    def halo_copy(slot):
        step_x, step_y = HELD[slot]
        if slot == 0:
            source, target = modes.at[:, 0], halo_x.reshape(3 * width, span_y, span_z)
        elif slot == 1:
            source, target = modes.at[:, :, 0], halo_y
        else:
            source, target = modes.at[:, 0, 0 if step_y > 0 else span_y - 1], halo_c.at[slot - 2]
        return pltpu.make_async_remote_copy(
            src_ref=source, dst_ref=target,
            send_sem=halo_send.at[slot], recv_sem=halo_recv.at[slot],
            device_id=where_is(-step_x, -step_y), device_id_type=MESH,
        )

    for slot, (step_x, step_y) in enumerate(RING):
        @pl.when(exists(-step_x, -step_y))
        def _():
            ring_copy(slot).start()
    for slot, (step_x, step_y) in enumerate(HELD):
        @pl.when(exists(-step_x, -step_y))
        def _():
            halo_copy(slot).start()

    for slot, (step_x, step_y) in enumerate(RING):
        @pl.when(jnp.logical_not(exists(step_x, step_y)))
        def _():
            target = ring_refs(slot)[1]
            target[...] = jnp.full(target.shape, -1, jnp.int32)
    for slot, (step_x, step_y) in enumerate(HELD):
        @pl.when(jnp.logical_not(exists(step_x, step_y)))
        def _():
            if slot == 0:
                halo_x[...] = jnp.zeros(halo_x.shape, jnp.float32)
            elif slot == 1:
                halo_y[...] = jnp.zeros(halo_y.shape, jnp.float32)
            else:
                halo_c[slot - 2] = jnp.zeros(halo_c.shape[1:], jnp.float32)

    def stiff_of(values):
        total = jnp.zeros(values.shape, jnp.float32)
        for level in range(stiff.shape[0]):
            total = jnp.where(values == level, stiff[level], total)
        return total

    load_region.wait()
    for x in range(span_x):
        sigma[1 + x, 1 : 1 + span_y] = stiff_of(cells[x])
    load_modes.wait()
    flat = field.reshape(3 * width * span_x * span_y, span_z)
    columns = 3 * span_x * span_y

    def column(comp, x, y):
        return flat[pl.ds((comp * span_x + x) * span_y + y, width, stride=columns), :]

    def plane(x):
        return [
            jnp.stack([column(comp, x, y) for y in range(span_y)]) for comp in range(3)
        ]

    for slot, (step_x, step_y) in enumerate(RING):
        @pl.when(exists(step_x, step_y))
        def _():
            ring_copy(slot).wait_recv()
    for side, x in ((0, 0), (1, span_x + 1)):
        sigma[x, 1 : 1 + span_y] = stiff_of(ring_row[side])
        low = stiff_of(ring_corner[2 * side])
        sigma[x, 0:1] = low[span_y - 1 : span_y]
        high = stiff_of(ring_corner[2 * side + 1])
        sigma[x, span_y + 1 : span_y + 2] = high[0:1]
    for x in range(span_x):
        low = stiff_of(ring_side[0, x])
        sigma[1 + x, 0:1] = low[span_y - 1 : span_y]
        high = stiff_of(ring_side[1, x])
        sigma[1 + x, span_y + 1 : span_y + 2] = high[0:1]

    def sigma_parts(x):
        level = {}
        for step in (-1, 0, 1):
            s = sigma[x, 1 + step : 1 + step + span_y]
            level[step] = (s,) + lane_steps(s)
        s0, e0, o0 = level[0]
        se, ee, oe = [level[1][i] + level[-1][i] for i in range(3)]
        so, eo, oo = [level[1][i] - level[-1][i] for i in range(3)]
        return s0, e0, o0, se, ee, oe, so, eo, oo

    parts = [sigma_parts(x) for x in range(span_x + 2)]
    for x in range(1, span_x + 1):
        s0, e0, o0, se, ee, oe, so, eo, oo = parts[x]
        fs, fe, fo, fse, fee, foe, fso, feo, foo = [
            parts[x + 1][i] + parts[x - 1][i] for i in range(9)
        ]
        ds, de, do, dse, dee, doe, dso, deo, doo = [
            parts[x + 1][i] - parts[x - 1][i] for i in range(9)
        ]
        plain = (
            (mass_share + DIAG_SUM) * s0
            + W1 * (e0 + se + fs) + W2 * (ee + fe + fse) + W3 * fee
        )
        xx = plain + B1 * fs + B2 * (fse + fe) + B3 * fee
        yy = plain + B1 * se + B2 * (fse + ee) + B3 * fee
        zz = plain + B1 * e0 + B2 * (fe + ee) + B3 * fee
        xy = B2 * dso + B3 * deo
        xz = B2 * do + B3 * doe
        yz = B2 * oo + B3 * foo
        for i, value in enumerate((xx, yy, zz, xy, xz, yz)):
            diag[i, x - 1] = 0.5 * value

    def spread(row):
        return jnp.broadcast_to(row, (width, span_z))

    def spread_sigma(x, low, high):
        return jnp.stack([spread(sigma[1 + x, 1 + y : 2 + y]) for y in range(low, high)])

    def spread_diag(i, x):
        return jnp.stack([spread(diag[i, x, y : y + 1]) for y in range(span_y)])

    own = jnp.zeros((2 * width, 2 * width), jnp.float32)
    here, before, after, fields, weights = [], [], [], [], []
    edge_here, edge_before, edge_after = [], [], []
    for x in range(span_x):
        last = x == span_x - 1
        v = plane(x)
        s = spread_sigma(x, 0, span_y)
        a, b, c = plane_parts(v, -1 if last else 0, span_y + 1)
        if last:
            beyond = c
            a, b = [[t[1:] for t in group_] for group_ in (a, b)]
            sv = [s * t for t in v]
            ea, eb, ec = plane_parts(sv, -1, span_y + 1)
            beyond_s = ec
            ea, eb = [[t[span_y + 1 :] for t in group_] for group_ in (ea, eb)]
        else:
            sv = [s[span_y - 1 :] * t[span_y - 1 :] for t in v]
            ea, eb, ec = plane_parts(sv, 1, 2)
        here.append(a); before.append(b); after.append(c)
        edge_here.append(ea); edge_before.append(eb); edge_after.append(ec)
        fields.append(v); weights.append(s)

    side = []
    for x in range(span_x):
        reach = list(here[x])
        edge = list(edge_here[x])
        if x + 1 < span_x:
            reach = [r + t for r, t in zip(reach, before[x + 1])]
            edge = [r + t for r, t in zip(edge, edge_before[x + 1])]
        if x > 0:
            reach = [r + t for r, t in zip(reach, after[x - 1])]
            edge = [r + t for r, t in zip(edge, edge_after[x - 1])]
        v, s = fields[x], weights[x]
        dxx, dyy, dzz, dxy, dxz, dyz = [spread_diag(i, x) for i in range(6)]
        applied = [
            dxx * v[0] + dxy * v[1] + dxz * v[2],
            dxy * v[0] + dyy * v[1] + dyz * v[2],
            dxz * v[0] + dyz * v[1] + dzz * v[2],
        ]
        for comp in range(3):
            left = applied[comp] - s * reach[comp][:span_y]
            own = own + product(stacked(left), stacked(v[comp]))
        s_side = spread_sigma(x, span_y, span_y + 1)
        side.append([stacked(s_side * reach[i][span_y:] + edge[i]) for i in range(3)])
    s_row = spread_sigma(span_x, -1, span_y + 1)
    row = [s_row * beyond[i] + beyond_s[i] for i in range(3)]
    row_mid = [stacked(t[1 : span_y + 1]) for t in row]
    row_low = [stacked(t[:1]) for t in row]
    row_high = [stacked(t[span_y + 1 :]) for t in row]
    block = folded(own, width)
    block = block + block.T

    for slot, (step_x, step_y) in enumerate(HELD):
        @pl.when(exists(step_x, step_y))
        def _():
            halo_copy(slot).wait_recv()

    def pair(left, right):
        total = product(left[0], right[0])
        for l, r in zip(left[1:], right[1:]):
            total = total + product(l, r)
        return -folded(total, width)

    flat_y = halo_y.reshape(3 * width * span_x, span_z)
    near_c = [
        [stacked(halo_c[i, pl.ds(comp, width, stride=3), :][None]) for comp in range(3)]
        for i in range(2)
    ]
    c_low = pair(row_low, near_c[0])
    c_high = pair(row_high, near_c[1])
    c_side = pair(
        [side[x][comp] for x in range(span_x) for comp in range(3)],
        [
            stacked(flat_y[pl.ds(comp * span_x + x, width, stride=3 * span_x), :][None])
            for x in range(span_x) for comp in range(3)
        ],
    )
    c_mid = pair(
        row_mid,
        [
            stacked(jnp.stack([
                halo_x[pl.ds(comp * span_y + y, width, stride=3 * span_y), :]
                for y in range(span_y)
            ]))
            for comp in range(3)
        ],
    )

    next_x = jnp.minimum(me_x + 1, count_x - 1)
    next_y = jnp.minimum(me_y + 1, count_y - 1)
    last_y = jnp.maximum(me_y - 1, 0)
    g_self, g_side = group[me_x, me_y], group[me_x, next_y]
    g_low, g_mid, g_high = group[next_x, last_y], group[next_x, me_y], group[next_x, next_y]
    slot_of = lax.broadcasted_iota(jnp.int32, (width, GROUPS * width), 1) // width

    def placed(value, label):
        return jnp.where(slot_of == label, jnp.concatenate([value] * GROUPS, axis=1), 0.0)

    level = placed(block, g_self) + placed(c_side, g_side)
    ahead = placed(c_low, g_low) + placed(c_mid, g_mid) + placed(c_high, g_high)
    strip = jnp.concatenate([level, ahead], axis=1)
    none = jnp.zeros_like(level)
    back_side = jnp.concatenate([placed(c_side.T, g_self), none], axis=1)
    backs = [
        (jnp.concatenate([placed(value.T, g_self), none], axis=1), label)
        for value, label in ((c_low, g_low), (c_mid, g_mid), (c_high, g_high))
    ]
    for g in range(GROUPS):
        part_a[g * width : (g + 1) * width] = (
            jnp.where(g_self == g, strip, 0.0) + jnp.where(g_side == g, back_side, 0.0)
        )
        total = jnp.zeros_like(strip)
        for value, label in backs:
            total = total + jnp.where(label == g, value, 0.0)
        part_b[g * width : (g + 1) * width] = total

    def rows_of(there):
        return pl.ds(pl.multiple_of(there * rows, rows), rows)

    def a_copy(other):
        there = lax.rem(me_y + other, count_y)
        return pltpu.make_async_remote_copy(
            src_ref=part_a.at[rows_of(there)], dst_ref=got_a.at[other],
            send_sem=a_send.at[other], recv_sem=a_recv.at[other],
            device_id={"gx": me_x, "gy": there}, device_id_type=MESH,
        )

    def b_copy(other):
        there = lax.rem(me_y + other, count_y)
        return pltpu.make_async_remote_copy(
            src_ref=part_b.at[rows_of(there)], dst_ref=got_b.at[other],
            send_sem=b_send.at[other], recv_sem=b_recv.at[other],
            device_id={"gx": me_x + 1, "gy": there}, device_id_type=MESH,
        )

    @pl.when(exists(1, 0))
    def _():
        for other in range(count_y):
            b_copy(other).start()

    for other in range(1, count_y):
        a_copy(other).start()

    @pl.when(jnp.logical_not(exists(-1, 0)))
    def _():
        got_b[...] = jnp.zeros(got_b.shape, jnp.float32)

    total = part_a[rows_of(me_y), :]
    for other in range(1, count_y):
        a_copy(other).wait_recv()
        total = total + got_a[other]
    out[0, :, GROUPS * width :] = total

    @pl.when(exists(-1, 0))
    def _():
        for other in range(count_y):
            b_copy(other).wait_recv()

    total = got_b[0]
    for other in range(1, count_y):
        total = total + got_b[other]
    out[0, :, : GROUPS * width] = total[:, : GROUPS * width]

    for slot, (step_x, step_y) in enumerate(RING):
        @pl.when(exists(-step_x, -step_y))
        def _():
            ring_copy(slot).wait_send()
    for slot, (step_x, step_y) in enumerate(HELD):
        @pl.when(exists(-step_x, -step_y))
        def _():
            halo_copy(slot).wait_send()
    for other in range(1, count_y):
        a_copy(other).wait_send()

    @pl.when(exists(1, 0))
    def _():
        for other in range(count_y):
            b_copy(other).wait_send()


def shards(counts, modes, region, stiffness, coarse_group):
    width, comps, span_x, span_y, span_z = modes.shape
    rows = GROUPS * width // counts[1]
    f32, i32 = jnp.float32, jnp.int32
    dma = pltpu.SemaphoreType.DMA
    lanes = 2 * GROUPS * width
    return pl.pallas_call(
        functools.partial(kernel, (width, span_x, span_y, span_z), counts),
        out_shape=jax.ShapeDtypeStruct((1, rows, 3 * GROUPS * width), f32),
        in_specs=[
            pl.BlockSpec(memory_space=pl.ANY),
            pl.BlockSpec(memory_space=pl.ANY),
            pl.BlockSpec(memory_space=pltpu.SMEM),
            pl.BlockSpec(memory_space=pltpu.SMEM),
        ],
        out_specs=pl.BlockSpec(memory_space=pltpu.VMEM),
        scratch_shapes=[
            pltpu.VMEM((comps * width, span_x, span_y, span_z), f32),
            pltpu.VMEM((span_x, span_y, span_z), i32),
            pltpu.VMEM((2, span_y, span_z), i32),
            pltpu.VMEM((2, span_x, span_y, span_z), i32),
            pltpu.VMEM((4, span_y, span_z), i32),
            pltpu.VMEM((span_x + 2, span_y + 8, span_z), f32),
            pltpu.VMEM((6, span_x, span_y, span_z), f32),
            pltpu.VMEM((comps * width * span_y, span_z), f32),
            pltpu.VMEM((comps * width, span_x, span_z), f32),
            pltpu.VMEM((2, comps * width, span_z), f32),
            pltpu.VMEM((GROUPS * width, lanes), f32),
            pltpu.VMEM((GROUPS * width, lanes), f32),
            pltpu.VMEM((counts[1], rows, lanes), f32),
            pltpu.VMEM((counts[1], rows, lanes), f32),
            dma((2,)),
            dma((len(RING),)), dma((len(RING),)),
            dma((len(HELD),)), dma((len(HELD),)),
            dma((counts[1],)), dma((counts[1],)),
            dma((counts[1],)), dma((counts[1],)),
        ],
        compiler_params=pltpu.CompilerParams(collective_id=0, has_side_effects=True),
    )(modes.reshape(width * comps, span_x, span_y, span_z), region, stiffness, coarse_group)


def solution(mesh):
    counts = (mesh.shape["gx"], mesh.shape["gy"])
    in_specs = (P(None, None, "gx", "gy", None), P("gx", "gy", None), P(), P())
    out_specs = P("gx", "gy", None)
    return jax.shard_map(
        functools.partial(shards, counts), mesh=mesh, in_specs=in_specs,
        out_specs=out_specs, check_vma=False,
    )
```

```python
import functools

import jax
import jax.numpy as jnp
from jax import lax
from jax.experimental import pallas as pl
from jax.experimental.pallas import tpu as pltpu
from jax.sharding import PartitionSpec as P

GROUPS = 4

beta_shear = 0.5
mass_share = 0.1

W1, W2, W3 = 0.5, 0.25, 0.125
B1, B2, B3 = W1 * beta_shear, W2 * beta_shear / 2, W3 * beta_shear / 3
DIAG_SUM = 6 * W1 + 12 * W2 + 8 * W3 + 2 * B1 + 8 * B2 + 8 * B3

MESH = pl.DeviceIdType.MESH
RING = [(-1, -1), (-1, 0), (-1, 1), (0, -1), (0, 1), (1, -1), (1, 0), (1, 1)]
HELD = [(1, -1), (1, 1), (0, 1), (1, 0), (1, 0), (1, 0)]


def lane_steps(value):
    lane = lax.broadcasted_iota(jnp.int32, value.shape, value.ndim - 1)
    size = value.shape[-1]
    before = jnp.where(lane == 0, 0.0, pltpu.roll(value, 1, value.ndim - 1))
    after = jnp.where(lane == size - 1, 0.0, pltpu.roll(value, size - 1, value.ndim - 1))
    return before + after, after - before


def plane_parts(fields, low, high):
    span = fields[0].shape[0]

    def at(value, step):
        first, last = low + step, high + step
        start, stop = min(max(first, 0), span), min(max(last, 0), span)
        zeros = lambda n: [jnp.zeros((n,) + value.shape[1:], value.dtype)] if n else []
        if start >= stop:
            return zeros(last - first)[0]
        pieces = zeros(start - first) + [value[start:stop]] + zeros(last - stop)
        return pieces[0] if len(pieces) == 1 else jnp.concatenate(pieces, axis=0)

    def even(value):
        return at(value, -1) + at(value, 1)

    def odd(value):
        return at(value, 1) - at(value, -1)

    vx, vy, vz = fields
    (ex, ox), (ey, oy), (ez, oz) = [lane_steps(v) for v in fields]
    level = at(W1 * ex, 0) + even(W1 * vx + W2 * ex)
    share = at((W1 + B1) * vx + (W2 + B2) * ex, 0) + even((W2 + B2) * vx + (W3 + B3) * ex)
    turn = odd(B2 * vy + B3 * ey) + B2 * at(oz, 0) + B3 * even(oz)
    out_x = (level, share + turn, share - turn)
    skew = odd(oz)
    level = at(W1 * ey, 0) + even((W1 + B1) * vy + (W2 + B2) * ey) + B2 * skew
    share = at(W1 * vy + W2 * ey, 0) + even((W2 + B2) * vy + (W3 + B3) * ey) + B3 * skew
    turn = odd(B2 * vx + B3 * ex)
    out_y = (level, share + turn, share - turn)
    skew = odd(oy)
    wide = W1 * vz + (W2 + B2) * ez
    level = at((W1 + B1) * ez, 0) + even(wide) + B2 * skew
    share = at(wide, 0) + even(W2 * vz + (W3 + B3) * ez) + B3 * skew
    turn = B2 * at(ox, 0) + B3 * even(ox)
    out_z = (level, share + turn, share - turn)
    here, before, after = zip(out_x, out_y, out_z)
    return here, before, after


def stacked(value):
    high = value.astype(jnp.bfloat16)
    low = (value - high.astype(jnp.float32)).astype(jnp.bfloat16)
    cells = value.shape[0]
    join = lambda part: jnp.concatenate([part[i] for i in range(cells)], axis=1)
    return jnp.concatenate([join(high), join(low)], axis=0)


def product(left, right):
    return lax.dot_general(
        left, right, (((1,), (1,)), ((), ())), preferred_element_type=jnp.float32
    )


def folded(value, width):
    value = value[:width] + value[width:]
    return value[:, :width] + value[:, width:]


def kernel(
    shape, counts, modes, region, stiff_in, group_in, out,
    stiff, group, field, cells, ring_row, ring_side, ring_corner, sigma, diag,
    halo_x, halo_y, halo_c, part_a, part_b, got_a, got_b,
    load_sem, ring_send, ring_recv, halo_send, halo_recv, a_send, a_recv, b_send, b_recv,
):
    width, span_x, span_y, span_z = shape
    count_x, count_y = counts
    rows = GROUPS * width // count_y
    me_x, me_y = lax.axis_index("gx"), lax.axis_index("gy")

    def exists(step_x, step_y):
        ok = me_x >= 0
        if step_x < 0:
            ok = jnp.logical_and(ok, me_x > 0)
        if step_x > 0:
            ok = jnp.logical_and(ok, me_x < count_x - 1)
        if step_y < 0:
            ok = jnp.logical_and(ok, me_y > 0)
        if step_y > 0:
            ok = jnp.logical_and(ok, me_y < count_y - 1)
        return ok

    def where_is(step_x, step_y):
        return {"gx": me_x + step_x, "gy": me_y + step_y}

    load_modes = pltpu.make_async_copy(modes, field, load_sem.at[0])
    load_region = pltpu.make_async_copy(region, cells, load_sem.at[1])
    load_stiff = pltpu.make_async_copy(stiff_in, stiff, load_sem.at[2])
    load_group = pltpu.make_async_copy(group_in, group, load_sem.at[3])

    barrier = pltpu.get_barrier_semaphore()
    for step_x in (-1, 0, 1):
        @pl.when(exists(step_x, 0))
        def _():
            for other in range(1 if step_x == 0 else 0, count_y):
                there = lax.rem(me_y + other, count_y)
                pl.semaphore_signal(
                    barrier, inc=1,
                    device_id={"gx": me_x + step_x, "gy": there}, device_id_type=MESH,
                )
    load_region.start()
    load_stiff.start()
    load_group.start()
    load_modes.start()
    strips = 1 + (me_x > 0).astype(jnp.int32) + (me_x < count_x - 1).astype(jnp.int32)
    pl.semaphore_wait(barrier, strips * count_y - 1)

    def ring_refs(slot):
        step_x, step_y = RING[slot]
        edge_x = 0 if step_x > 0 else span_x - 1
        edge_y = 0 if step_y > 0 else span_y - 1
        if step_x == 0:
            return region.at[:, edge_y], ring_side.at[(step_y + 1) // 2]
        if step_y == 0:
            return region.at[edge_x], ring_row.at[(step_x + 1) // 2]
        return region.at[edge_x, edge_y], ring_corner.at[(step_x + 1) + (step_y + 1) // 2]

    def ring_copy(slot):
        step_x, step_y = RING[slot]
        source, target = ring_refs(slot)
        return pltpu.make_async_remote_copy(
            src_ref=source, dst_ref=target,
            send_sem=ring_send.at[slot], recv_sem=ring_recv.at[slot],
            device_id=where_is(-step_x, -step_y), device_id_type=MESH,
        )

    def halo_copy(slot):
        step_x, step_y = HELD[slot]
        if slot < 2:
            merged = modes.reshape(3 * width, span_x, span_y, span_z)
            source, target = merged.at[:, 0, 0 if step_y > 0 else span_y - 1], halo_c.at[slot]
        elif slot == 2:
            source, target = modes.at[:, :, :, 0], halo_y
        else:
            source, target = modes.at[:, slot - 3, 0], halo_x.at[slot - 3]
        return pltpu.make_async_remote_copy(
            src_ref=source, dst_ref=target,
            send_sem=halo_send.at[slot], recv_sem=halo_recv.at[slot],
            device_id=where_is(-step_x, -step_y), device_id_type=MESH,
        )

    for slot, (step_x, step_y) in enumerate(RING):
        @pl.when(exists(-step_x, -step_y))
        def _():
            ring_copy(slot).start()
    for slot, (step_x, step_y) in enumerate(HELD):
        @pl.when(exists(-step_x, -step_y))
        def _():
            halo_copy(slot).start()

    for slot, (step_x, step_y) in enumerate(RING):
        @pl.when(jnp.logical_not(exists(step_x, step_y)))
        def _():
            target = ring_refs(slot)[1]
            target[...] = jnp.full(target.shape, -1, jnp.int32)
    for slot, (step_x, step_y) in enumerate(HELD):
        @pl.when(jnp.logical_not(exists(step_x, step_y)))
        def _():
            target = halo_c.at[slot] if slot < 2 else halo_y if slot == 2 else halo_x.at[slot - 3]
            target[...] = jnp.zeros(target.shape, jnp.float32)

    def stiff_of(values):
        total = jnp.zeros(values.shape, jnp.float32)
        for level in range(stiff.shape[0]):
            total = jnp.where(values == level, stiff[level], total)
        return total

    load_stiff.wait()
    load_group.wait()
    load_region.wait()
    for x in range(span_x):
        sigma[1 + x, 1 : 1 + span_y] = stiff_of(cells[x])
    load_modes.wait()
    flat = field.reshape(3 * width * span_x * span_y, span_z)
    columns = 3 * span_x * span_y

    def column(comp, x, y):
        return flat[pl.ds((comp * span_x + x) * span_y + y, width, stride=columns), :]

    def plane(x):
        return [
            jnp.stack([column(comp, x, y) for y in range(span_y)]) for comp in range(3)
        ]

    for slot, (step_x, step_y) in enumerate(RING):
        @pl.when(exists(step_x, step_y))
        def _():
            ring_copy(slot).wait_recv()
    for side, x in ((0, 0), (1, span_x + 1)):
        sigma[x, 1 : 1 + span_y] = stiff_of(ring_row[side])
        sigma[x, 0:1] = stiff_of(ring_corner[2 * side : 2 * side + 1])
        sigma[x, span_y + 1 : span_y + 2] = stiff_of(ring_corner[2 * side + 1 : 2 * side + 2])
    low, high = stiff_of(ring_side[0]), stiff_of(ring_side[1])
    for x in range(span_x):
        sigma[1 + x, 0:1] = low[x : x + 1]
        sigma[1 + x, span_y + 1 : span_y + 2] = high[x : x + 1]

    def sigma_parts(x):
        level = {}
        for step in (-1, 0, 1):
            s = sigma[x, 1 + step : 1 + step + span_y]
            level[step] = (s,) + lane_steps(s)
        s0, e0, o0 = level[0]
        se, ee, oe = [level[1][i] + level[-1][i] for i in range(3)]
        so, eo, oo = [level[1][i] - level[-1][i] for i in range(3)]
        return s0, e0, o0, se, ee, oe, so, eo, oo

    parts = [sigma_parts(x) for x in range(span_x + 2)]
    for x in range(1, span_x + 1):
        s0, e0, o0, se, ee, oe, so, eo, oo = parts[x]
        fs, fe, fo, fse, fee, foe, fso, feo, foo = [
            parts[x + 1][i] + parts[x - 1][i] for i in range(9)
        ]
        ds, de, do, dse, dee, doe, dso, deo, doo = [
            parts[x + 1][i] - parts[x - 1][i] for i in range(9)
        ]
        plain = (
            (mass_share + DIAG_SUM) * s0
            + W1 * (e0 + se + fs) + W2 * (ee + fe + fse) + W3 * fee
        )
        xx = plain + B1 * fs + B2 * (fse + fe) + B3 * fee
        yy = plain + B1 * se + B2 * (fse + ee) + B3 * fee
        zz = plain + B1 * e0 + B2 * (fe + ee) + B3 * fee
        xy = B2 * dso + B3 * deo
        xz = B2 * do + B3 * doe
        yz = B2 * oo + B3 * foo
        for i, value in enumerate((xx, yy, zz, xy, xz, yz)):
            diag[i, x - 1] = 0.5 * value

    def spread(row):
        return jnp.broadcast_to(row, (width, span_z))

    def spread_sigma(x, low, high):
        return jnp.stack([spread(sigma[1 + x, 1 + y : 2 + y]) for y in range(low, high)])

    def spread_diag(i, x):
        return jnp.stack([spread(diag[i, x, y : y + 1]) for y in range(span_y)])

    own = jnp.zeros((2 * width, 2 * width), jnp.float32)
    here, before, after, fields, weights = [], [], [], [], []
    edge_here, edge_before, edge_after = [], [], []
    for x in range(span_x):
        last = x == span_x - 1
        v = plane(x)
        s = spread_sigma(x, 0, span_y)
        a, b, c = plane_parts(v, -1 if last else 0, span_y + 1)
        if last:
            beyond = c
            a, b = [[t[1:] for t in group_] for group_ in (a, b)]
            sv = [s * t for t in v]
            ea, eb, ec = plane_parts(sv, -1, span_y + 1)
            beyond_s = ec
            ea, eb = [[t[span_y + 1 :] for t in group_] for group_ in (ea, eb)]
        else:
            sv = [s[span_y - 1 :] * t[span_y - 1 :] for t in v]
            ea, eb, ec = plane_parts(sv, 1, 2)
        here.append(a); before.append(b); after.append(c)
        edge_here.append(ea); edge_before.append(eb); edge_after.append(ec)
        fields.append(v); weights.append(s)

    side = []
    for x in range(span_x):
        reach = list(here[x])
        edge = list(edge_here[x])
        if x + 1 < span_x:
            reach = [r + t for r, t in zip(reach, before[x + 1])]
            edge = [r + t for r, t in zip(edge, edge_before[x + 1])]
        if x > 0:
            reach = [r + t for r, t in zip(reach, after[x - 1])]
            edge = [r + t for r, t in zip(edge, edge_after[x - 1])]
        v, s = fields[x], weights[x]
        dxx, dyy, dzz, dxy, dxz, dyz = [spread_diag(i, x) for i in range(6)]
        applied = [
            dxx * v[0] + dxy * v[1] + dxz * v[2],
            dxy * v[0] + dyy * v[1] + dyz * v[2],
            dxz * v[0] + dyz * v[1] + dzz * v[2],
        ]
        for comp in range(3):
            left = applied[comp] - s * reach[comp][:span_y]
            own = own + product(stacked(left), stacked(v[comp]))
        s_side = spread_sigma(x, span_y, span_y + 1)
        side.append([stacked(s_side * reach[i][span_y:] + edge[i]) for i in range(3)])
    s_row = spread_sigma(span_x, -1, span_y + 1)
    row = [s_row * beyond[i] + beyond_s[i] for i in range(3)]
    row_mid = [stacked(t[1 : span_y + 1]) for t in row]
    row_low = [stacked(t[:1]) for t in row]
    row_high = [stacked(t[span_y + 1 :]) for t in row]
    block = folded(own, width)
    block = block + block.T

    def arrived(slot):
        @pl.when(exists(*HELD[slot]))
        def _():
            halo_copy(slot).wait_recv()

    def pair(left, right):
        total = product(left[0], right[0])
        for l, r in zip(left[1:], right[1:]):
            total = total + product(l, r)
        return total

    def corner(i):
        return [stacked(halo_c[i, pl.ds(comp, width, stride=3), :][None]) for comp in range(3)]

    arrived(2)
    flat_y = halo_y.reshape(3 * width * span_x, span_z)
    c_side = -folded(pair(
        [side[x][comp] for x in range(span_x) for comp in range(3)],
        [
            stacked(flat_y[pl.ds(comp * span_x + x, width, stride=3 * span_x), :][None])
            for x in range(span_x) for comp in range(3)
        ],
    ), width)
    arrived(0)
    c_low = -folded(pair(row_low, corner(0)), width)
    arrived(1)
    c_high = -folded(pair(row_high, corner(1)), width)
    c_mid = jnp.zeros((2 * width, 2 * width), jnp.float32)
    for comp in range(3):
        arrived(3 + comp)
        flat_x = halo_x.at[comp].reshape(width * span_y, span_z)
        near = jnp.stack([flat_x[pl.ds(y, width, stride=span_y), :] for y in range(span_y)])
        c_mid = c_mid + product(row_mid[comp], stacked(near))
    c_mid = -folded(c_mid, width)

    next_x = jnp.minimum(me_x + 1, count_x - 1)
    next_y = jnp.minimum(me_y + 1, count_y - 1)
    last_y = jnp.maximum(me_y - 1, 0)
    g_self, g_side = group[me_y, me_x], group[next_y, me_x]
    g_low, g_mid, g_high = group[last_y, next_x], group[me_y, next_x], group[next_y, next_x]
    slot_of = lax.broadcasted_iota(jnp.int32, (width, GROUPS * width), 1) // width

    def placed(value, label):
        return jnp.where(slot_of == label, jnp.concatenate([value] * GROUPS, axis=1), 0.0)

    level = placed(block, g_self) + placed(c_side, g_side)
    ahead = placed(c_low, g_low) + placed(c_mid, g_mid) + placed(c_high, g_high)
    strip = jnp.concatenate([level, ahead], axis=1)
    none = jnp.zeros_like(level)
    back_side = jnp.concatenate([placed(c_side.T, g_self), none], axis=1)
    backs = [
        (jnp.concatenate([placed(value.T, g_self), none], axis=1), label)
        for value, label in ((c_low, g_low), (c_mid, g_mid), (c_high, g_high))
    ]
    for g in range(GROUPS):
        part_a[g * width : (g + 1) * width] = (
            jnp.where(g_self == g, strip, 0.0) + jnp.where(g_side == g, back_side, 0.0)
        )
        total = jnp.zeros_like(strip)
        for value, label in backs:
            total = total + jnp.where(label == g, value, 0.0)
        part_b[g * width : (g + 1) * width] = total

    def rows_of(there):
        return pl.ds(pl.multiple_of(there * rows, rows), rows)

    def a_copy(other):
        there = lax.rem(me_y + other, count_y)
        return pltpu.make_async_remote_copy(
            src_ref=part_a.at[rows_of(there)], dst_ref=got_a.at[other],
            send_sem=a_send.at[other], recv_sem=a_recv.at[other],
            device_id={"gx": me_x, "gy": there}, device_id_type=MESH,
        )

    def b_copy(other):
        there = lax.rem(me_y + other, count_y)
        return pltpu.make_async_remote_copy(
            src_ref=part_b.at[rows_of(there)], dst_ref=got_b.at[other],
            send_sem=b_send.at[other], recv_sem=b_recv.at[other],
            device_id={"gx": me_x + 1, "gy": there}, device_id_type=MESH,
        )

    @pl.when(exists(1, 0))
    def _():
        for other in range(count_y):
            b_copy(other).start()

    for other in range(1, count_y):
        a_copy(other).start()

    @pl.when(jnp.logical_not(exists(-1, 0)))
    def _():
        got_b[...] = jnp.zeros(got_b.shape, jnp.float32)

    total = part_a[rows_of(me_y), :]
    for other in range(1, count_y):
        a_copy(other).wait_recv()
        total = total + got_a[other]
    out[0, :, GROUPS * width :] = total

    @pl.when(exists(-1, 0))
    def _():
        for other in range(count_y):
            b_copy(other).wait_recv()

    total = got_b[0]
    for other in range(1, count_y):
        total = total + got_b[other]
    out[0, :, : GROUPS * width] = total[:, : GROUPS * width]

    for slot, (step_x, step_y) in enumerate(RING):
        @pl.when(exists(-step_x, -step_y))
        def _():
            ring_copy(slot).wait_send()
    for slot, (step_x, step_y) in enumerate(HELD):
        @pl.when(exists(-step_x, -step_y))
        def _():
            halo_copy(slot).wait_send()
    for other in range(1, count_y):
        a_copy(other).wait_send()

    @pl.when(exists(1, 0))
    def _():
        for other in range(count_y):
            b_copy(other).wait_send()


def shards(counts, modes, region, stiffness, coarse_group):
    width, comps, span_x, span_y, span_z = modes.shape
    rows = GROUPS * width // counts[1]
    f32, i32 = jnp.float32, jnp.int32
    dma = pltpu.SemaphoreType.DMA
    lanes = 2 * GROUPS * width
    return pl.pallas_call(
        functools.partial(kernel, (width, span_x, span_y, span_z), counts),
        out_shape=jax.ShapeDtypeStruct((1, rows, 3 * GROUPS * width), f32),
        in_specs=[
            pl.BlockSpec(memory_space=pltpu.HBM),
            pl.BlockSpec(memory_space=pltpu.HBM),
            pl.BlockSpec(memory_space=pltpu.HBM),
            pl.BlockSpec(memory_space=pltpu.HBM),
        ],
        out_specs=pl.BlockSpec(memory_space=pltpu.VMEM),
        scratch_shapes=[
            pltpu.SMEM(stiffness.shape, f32),
            pltpu.SMEM(coarse_group.shape[::-1], i32),
            pltpu.VMEM((width, comps, span_x, span_y, span_z), f32),
            pltpu.VMEM((span_x, span_y, span_z), i32),
            pltpu.VMEM((2, span_y, span_z), i32),
            pltpu.VMEM((2, span_x, span_z), i32),
            pltpu.VMEM((4, span_z), i32),
            pltpu.VMEM((span_x + 2, span_y + 8, span_z), f32),
            pltpu.VMEM((6, span_x, span_y, span_z), f32),
            pltpu.VMEM((comps, width, span_y, span_z), f32),
            pltpu.VMEM((width, comps, span_x, span_z), f32),
            pltpu.VMEM((2, comps * width, span_z), f32),
            pltpu.VMEM((GROUPS * width, lanes), f32),
            pltpu.VMEM((GROUPS * width, lanes), f32),
            pltpu.VMEM((counts[1], rows, lanes), f32),
            pltpu.VMEM((counts[1], rows, lanes), f32),
            dma((4,)),
            dma((len(RING),)), dma((len(RING),)),
            dma((len(HELD),)), dma((len(HELD),)),
            dma((counts[1],)), dma((counts[1],)),
            dma((counts[1],)), dma((counts[1],)),
        ],
        compiler_params=pltpu.CompilerParams(collective_id=0, has_side_effects=True),
    )(modes, region, stiffness, coarse_group.T)


def solution(mesh):
    counts = (mesh.shape["gx"], mesh.shape["gy"])
    in_specs = (P(None, None, "gx", "gy", None), P("gx", "gy", None), P(), P())
    out_specs = P("gx", "gy", None)
    return jax.shard_map(
        functools.partial(shards, counts), mesh=mesh, in_specs=in_specs,
        out_specs=out_specs, check_vma=False,
    )
```

```python
import functools

import jax
import jax.numpy as jnp
from jax import lax
from jax.experimental import pallas as pl
from jax.experimental.pallas import tpu as pltpu
from jax.sharding import PartitionSpec as P

GROUPS = 4

beta_shear = 0.5
mass_share = 0.1

W1, W2, W3 = 0.5, 0.25, 0.125
B1, B2, B3 = W1 * beta_shear, W2 * beta_shear / 2, W3 * beta_shear / 3
DIAG_SUM = 6 * W1 + 12 * W2 + 8 * W3 + 2 * B1 + 8 * B2 + 8 * B3

MESH = pl.DeviceIdType.MESH
RING = [(-1, -1), (-1, 0), (-1, 1), (0, -1), (0, 1), (1, -1), (1, 0), (1, 1)]
HELD = [(1, -1), (1, 1), (0, 1), (1, 0), (1, 0), (1, 0)]


def lane_steps(value):
    lane = lax.broadcasted_iota(jnp.int32, value.shape, value.ndim - 1)
    size = value.shape[-1]
    before = jnp.where(lane == 0, 0.0, pltpu.roll(value, 1, value.ndim - 1))
    after = jnp.where(lane == size - 1, 0.0, pltpu.roll(value, size - 1, value.ndim - 1))
    return before + after, after - before


def plane_parts(fields, low, high):
    span = fields[0].shape[0]

    def at(value, step):
        first, last = low + step, high + step
        start, stop = min(max(first, 0), span), min(max(last, 0), span)
        zeros = lambda n: [jnp.zeros((n,) + value.shape[1:], value.dtype)] if n else []
        if start >= stop:
            return zeros(last - first)[0]
        pieces = zeros(start - first) + [value[start:stop]] + zeros(last - stop)
        return pieces[0] if len(pieces) == 1 else jnp.concatenate(pieces, axis=0)

    def even(value):
        return at(value, -1) + at(value, 1)

    def odd(value):
        return at(value, 1) - at(value, -1)

    vx, vy, vz = fields
    (ex, ox), (ey, oy), (ez, oz) = [lane_steps(v) for v in fields]
    level = at(W1 * ex, 0) + even(W1 * vx + W2 * ex)
    share = at((W1 + B1) * vx + (W2 + B2) * ex, 0) + even((W2 + B2) * vx + (W3 + B3) * ex)
    turn = odd(B2 * vy + B3 * ey) + B2 * at(oz, 0) + B3 * even(oz)
    out_x = (level, share + turn, share - turn)
    skew = odd(oz)
    level = at(W1 * ey, 0) + even((W1 + B1) * vy + (W2 + B2) * ey) + B2 * skew
    share = at(W1 * vy + W2 * ey, 0) + even((W2 + B2) * vy + (W3 + B3) * ey) + B3 * skew
    turn = odd(B2 * vx + B3 * ex)
    out_y = (level, share + turn, share - turn)
    skew = odd(oy)
    wide = W1 * vz + (W2 + B2) * ez
    level = at((W1 + B1) * ez, 0) + even(wide) + B2 * skew
    share = at(wide, 0) + even(W2 * vz + (W3 + B3) * ez) + B3 * skew
    turn = B2 * at(ox, 0) + B3 * even(ox)
    out_z = (level, share + turn, share - turn)
    here, before, after = zip(out_x, out_y, out_z)
    return here, before, after


def stacked(value):
    high = value.astype(jnp.bfloat16)
    low = (value - high.astype(jnp.float32)).astype(jnp.bfloat16)
    cells = value.shape[0]
    join = lambda part: jnp.concatenate([part[i] for i in range(cells)], axis=1)
    return jnp.concatenate([join(high), join(low)], axis=0)


def product(left, right):
    return lax.dot_general(
        left, right, (((1,), (1,)), ((), ())), preferred_element_type=jnp.float32
    )


def folded(value, width):
    value = value[:width] + value[width:]
    return value[:, :width] + value[:, width:]


def kernel(
    shape, counts, modes, region, stiff_in, group_in, out,
    stiff, group, field, cells, ring_row, ring_side, ring_corner, sigma, diag,
    halo_x, halo_y, halo_c, part_a, part_b, got_a, got_b,
    load_sem, ring_send, ring_recv, halo_send, halo_recv, a_send, a_recv, b_send, b_recv,
):
    width, span_x, span_y, span_z = shape
    count_x, count_y = counts
    rows = GROUPS * width // count_y
    me_x, me_y = lax.axis_index("gx"), lax.axis_index("gy")

    def exists(step_x, step_y):
        ok = me_x >= 0
        if step_x < 0:
            ok = jnp.logical_and(ok, me_x > 0)
        if step_x > 0:
            ok = jnp.logical_and(ok, me_x < count_x - 1)
        if step_y < 0:
            ok = jnp.logical_and(ok, me_y > 0)
        if step_y > 0:
            ok = jnp.logical_and(ok, me_y < count_y - 1)
        return ok

    def where_is(step_x, step_y):
        return {"gx": me_x + step_x, "gy": me_y + step_y}

    load_modes = pltpu.make_async_copy(modes, field, load_sem.at[0])
    load_region = pltpu.make_async_copy(region, cells, load_sem.at[1])
    load_stiff = pltpu.make_async_copy(stiff_in, stiff, load_sem.at[2])
    load_group = pltpu.make_async_copy(group_in, group, load_sem.at[3])

    barrier = pltpu.get_barrier_semaphore()
    for step_x in (-1, 0, 1):
        @pl.when(exists(step_x, 0))
        def _():
            for other in range(1 if step_x == 0 else 0, count_y):
                there = lax.rem(me_y + other, count_y)
                pl.semaphore_signal(
                    barrier, inc=1,
                    device_id={"gx": me_x + step_x, "gy": there}, device_id_type=MESH,
                )
    load_region.start()
    load_stiff.start()
    load_group.start()
    load_modes.start()
    strips = 1 + (me_x > 0).astype(jnp.int32) + (me_x < count_x - 1).astype(jnp.int32)
    pl.semaphore_wait(barrier, strips * count_y - 1)

    def ring_refs(slot):
        step_x, step_y = RING[slot]
        edge_x = 0 if step_x > 0 else span_x - 1
        edge_y = 0 if step_y > 0 else span_y - 1
        if step_x == 0:
            return region.at[:, edge_y], ring_side.at[(step_y + 1) // 2]
        if step_y == 0:
            return region.at[edge_x], ring_row.at[(step_x + 1) // 2]
        return region.at[edge_x, edge_y], ring_corner.at[(step_x + 1) + (step_y + 1) // 2]

    def ring_copy(slot):
        step_x, step_y = RING[slot]
        source, target = ring_refs(slot)
        return pltpu.make_async_remote_copy(
            src_ref=source, dst_ref=target,
            send_sem=ring_send.at[slot], recv_sem=ring_recv.at[slot],
            device_id=where_is(-step_x, -step_y), device_id_type=MESH,
        )

    def halo_copy(slot):
        step_x, step_y = HELD[slot]
        if slot < 2:
            merged = modes.reshape(3 * width, span_x, span_y, span_z)
            source, target = merged.at[:, 0, 0 if step_y > 0 else span_y - 1], halo_c.at[slot]
        elif slot == 2:
            source, target = modes.at[:, :, :, 0], halo_y
        else:
            source, target = modes.at[:, slot - 3, 0], halo_x.at[slot - 3]
        return pltpu.make_async_remote_copy(
            src_ref=source, dst_ref=target,
            send_sem=halo_send.at[slot], recv_sem=halo_recv.at[slot],
            device_id=where_is(-step_x, -step_y), device_id_type=MESH,
        )

    for slot, (step_x, step_y) in enumerate(RING):
        @pl.when(exists(-step_x, -step_y))
        def _():
            ring_copy(slot).start()
    for slot, (step_x, step_y) in enumerate(HELD):
        @pl.when(exists(-step_x, -step_y))
        def _():
            halo_copy(slot).start()

    for slot, (step_x, step_y) in enumerate(RING):
        @pl.when(jnp.logical_not(exists(step_x, step_y)))
        def _():
            target = ring_refs(slot)[1]
            target[...] = jnp.full(target.shape, -1, jnp.int32)
    for slot, (step_x, step_y) in enumerate(HELD):
        @pl.when(jnp.logical_not(exists(step_x, step_y)))
        def _():
            target = halo_c.at[slot] if slot < 2 else halo_y if slot == 2 else halo_x.at[slot - 3]
            target[...] = jnp.zeros(target.shape, jnp.float32)

    def stiff_of(values):
        total = jnp.zeros(values.shape, jnp.float32)
        for level in range(stiff.shape[0]):
            total = jnp.where(values == level, stiff[level], total)
        return total

    load_stiff.wait()
    load_group.wait()
    load_region.wait()
    for x in range(span_x):
        sigma[1 + x, 1 : 1 + span_y] = stiff_of(cells[x])
    load_modes.wait()
    flat = field.reshape(3 * width * span_x * span_y, span_z)
    columns = 3 * span_x * span_y

    def column(comp, x, y):
        return flat[pl.ds((comp * span_x + x) * span_y + y, width, stride=columns), :]

    def plane(x):
        return [
            jnp.stack([column(comp, x, y) for y in range(span_y)]) for comp in range(3)
        ]

    for slot, (step_x, step_y) in enumerate(RING):
        @pl.when(exists(step_x, step_y))
        def _():
            ring_copy(slot).wait_recv()
    for side, x in ((0, 0), (1, span_x + 1)):
        sigma[x, 1 : 1 + span_y] = stiff_of(ring_row[side])
        sigma[x, 0:1] = stiff_of(ring_corner[2 * side : 2 * side + 1])
        sigma[x, span_y + 1 : span_y + 2] = stiff_of(ring_corner[2 * side + 1 : 2 * side + 2])
    low, high = stiff_of(ring_side[0]), stiff_of(ring_side[1])
    for x in range(span_x):
        sigma[1 + x, 0:1] = low[x : x + 1]
        sigma[1 + x, span_y + 1 : span_y + 2] = high[x : x + 1]

    def sigma_parts(x):
        level = {}
        for step in (-1, 0, 1):
            s = sigma[x, 1 + step : 1 + step + span_y]
            level[step] = (s,) + lane_steps(s)
        s0, e0, o0 = level[0]
        se, ee, oe = [level[1][i] + level[-1][i] for i in range(3)]
        so, eo, oo = [level[1][i] - level[-1][i] for i in range(3)]
        return s0, e0, o0, se, ee, oe, so, eo, oo

    parts = [sigma_parts(x) for x in range(span_x + 2)]
    for x in range(1, span_x + 1):
        s0, e0, o0, se, ee, oe, so, eo, oo = parts[x]
        fs, fe, fo, fse, fee, foe, fso, feo, foo = [
            parts[x + 1][i] + parts[x - 1][i] for i in range(9)
        ]
        ds, de, do, dse, dee, doe, dso, deo, doo = [
            parts[x + 1][i] - parts[x - 1][i] for i in range(9)
        ]
        plain = (
            (mass_share + DIAG_SUM) * s0
            + W1 * (e0 + se + fs) + W2 * (ee + fe + fse) + W3 * fee
        )
        xx = plain + B1 * fs + B2 * (fse + fe) + B3 * fee
        yy = plain + B1 * se + B2 * (fse + ee) + B3 * fee
        zz = plain + B1 * e0 + B2 * (fe + ee) + B3 * fee
        xy = B2 * dso + B3 * deo
        xz = B2 * do + B3 * doe
        yz = B2 * oo + B3 * foo
        for i, value in enumerate((xx, yy, zz, xy, xz, yz)):
            diag[i, x - 1] = 0.5 * value

    def spread(row):
        return jnp.broadcast_to(row, (width, span_z))

    def spread_sigma(x, low, high):
        return jnp.stack([spread(sigma[1 + x, 1 + y : 2 + y]) for y in range(low, high)])

    def spread_diag(i, x):
        return jnp.stack([spread(diag[i, x, y : y + 1]) for y in range(span_y)])

    own = jnp.zeros((2 * width, 2 * width), jnp.float32)
    here, before, after, fields, weights = [], [], [], [], []
    edge_here, edge_before, edge_after = [], [], []
    for x in range(span_x):
        last = x == span_x - 1
        v = plane(x)
        s = spread_sigma(x, 0, span_y)
        a, b, c = plane_parts(v, -1 if last else 0, span_y + 1)
        if last:
            beyond = c
            a, b = [[t[1:] for t in group_] for group_ in (a, b)]
            sv = [s * t for t in v]
            ea, eb, ec = plane_parts(sv, -1, span_y + 1)
            beyond_s = ec
            ea, eb = [[t[span_y + 1 :] for t in group_] for group_ in (ea, eb)]
        else:
            sv = [s[span_y - 1 :] * t[span_y - 1 :] for t in v]
            ea, eb, ec = plane_parts(sv, 1, 2)
        here.append(a); before.append(b); after.append(c)
        edge_here.append(ea); edge_before.append(eb); edge_after.append(ec)
        fields.append(v); weights.append(s)

    side = []
    for x in range(span_x):
        reach = list(here[x])
        edge = list(edge_here[x])
        if x + 1 < span_x:
            reach = [r + t for r, t in zip(reach, before[x + 1])]
            edge = [r + t for r, t in zip(edge, edge_before[x + 1])]
        if x > 0:
            reach = [r + t for r, t in zip(reach, after[x - 1])]
            edge = [r + t for r, t in zip(edge, edge_after[x - 1])]
        v, s = fields[x], weights[x]
        dxx, dyy, dzz, dxy, dxz, dyz = [spread_diag(i, x) for i in range(6)]
        applied = [
            dxx * v[0] + dxy * v[1] + dxz * v[2],
            dxy * v[0] + dyy * v[1] + dyz * v[2],
            dxz * v[0] + dyz * v[1] + dzz * v[2],
        ]
        for comp in range(3):
            left = applied[comp] - s * reach[comp][:span_y]
            own = own + product(stacked(left), stacked(v[comp]))
        s_side = spread_sigma(x, span_y, span_y + 1)
        side.append([stacked(s_side * reach[i][span_y:] + edge[i]) for i in range(3)])
    s_row = spread_sigma(span_x, -1, span_y + 1)
    row = [s_row * beyond[i] + beyond_s[i] for i in range(3)]
    row_mid = [stacked(t[1 : span_y + 1]) for t in row]
    row_low = [stacked(t[:1]) for t in row]
    row_high = [stacked(t[span_y + 1 :]) for t in row]
    block = folded(own, width)
    block = block + block.T

    def arrived(slot):
        @pl.when(exists(*HELD[slot]))
        def _():
            halo_copy(slot).wait_recv()

    def pair(left, right):
        total = product(left[0], right[0])
        for l, r in zip(left[1:], right[1:]):
            total = total + product(l, r)
        return total

    def corner(i):
        return [stacked(halo_c[i, pl.ds(comp, width, stride=3), :][None]) for comp in range(3)]

    arrived(2)
    flat_y = halo_y.reshape(3 * width * span_x, span_z)
    c_side = -folded(pair(
        [side[x][comp] for x in range(span_x) for comp in range(3)],
        [
            stacked(flat_y[pl.ds(comp * span_x + x, width, stride=3 * span_x), :][None])
            for x in range(span_x) for comp in range(3)
        ],
    ), width)
    arrived(0)
    c_low = -folded(pair(row_low, corner(0)), width)
    arrived(1)
    c_high = -folded(pair(row_high, corner(1)), width)
    c_mid = jnp.zeros((2 * width, 2 * width), jnp.float32)
    for comp in range(3):
        arrived(3 + comp)
        flat_x = halo_x.at[comp].reshape(width * span_y, span_z)
        near = jnp.stack([flat_x[pl.ds(y, width, stride=span_y), :] for y in range(span_y)])
        c_mid = c_mid + product(row_mid[comp], stacked(near))
    c_mid = -folded(c_mid, width)

    next_x = jnp.minimum(me_x + 1, count_x - 1)
    next_y = jnp.minimum(me_y + 1, count_y - 1)
    last_y = jnp.maximum(me_y - 1, 0)
    g_self, g_side = group[me_y, me_x], group[next_y, me_x]
    g_low, g_mid, g_high = group[last_y, next_x], group[me_y, next_x], group[next_y, next_x]
    slot_of = lax.broadcasted_iota(jnp.int32, (width, GROUPS * width), 1) // width

    def placed(value, label):
        return jnp.where(slot_of == label, jnp.concatenate([value] * GROUPS, axis=1), 0.0)

    level = placed(block, g_self) + placed(c_side, g_side)
    ahead = placed(c_low, g_low) + placed(c_mid, g_mid) + placed(c_high, g_high)
    strip = jnp.concatenate([level, ahead], axis=1)
    none = jnp.zeros_like(level)
    back_side = jnp.concatenate([placed(c_side.T, g_self), none], axis=1)
    backs = [
        (jnp.concatenate([placed(value.T, g_self), none], axis=1), label)
        for value, label in ((c_low, g_low), (c_mid, g_mid), (c_high, g_high))
    ]
    for g in range(GROUPS):
        part_a[g * width : (g + 1) * width] = (
            jnp.where(g_self == g, strip, 0.0) + jnp.where(g_side == g, back_side, 0.0)
        )
        total = jnp.zeros_like(strip)
        for value, label in backs:
            total = total + jnp.where(label == g, value, 0.0)
        part_b[g * width : (g + 1) * width] = total

    def rows_of(there):
        return pl.ds(pl.multiple_of(there * rows, rows), rows)

    def a_copy(other):
        there = lax.rem(me_y + other, count_y)
        return pltpu.make_async_remote_copy(
            src_ref=part_a.at[rows_of(there)], dst_ref=got_a.at[other],
            send_sem=a_send.at[other], recv_sem=a_recv.at[other],
            device_id={"gx": me_x, "gy": there}, device_id_type=MESH,
        )

    def b_copy(other):
        there = lax.rem(me_y + other, count_y)
        return pltpu.make_async_remote_copy(
            src_ref=part_b.at[rows_of(there)], dst_ref=got_b.at[other],
            send_sem=b_send.at[other], recv_sem=b_recv.at[other],
            device_id={"gx": me_x + 1, "gy": there}, device_id_type=MESH,
        )

    @pl.when(exists(1, 0))
    def _():
        for other in range(count_y):
            b_copy(other).start()

    for other in range(1, count_y):
        a_copy(other).start()

    @pl.when(jnp.logical_not(exists(-1, 0)))
    def _():
        got_b[...] = jnp.zeros(got_b.shape, jnp.float32)

    total = part_a[rows_of(me_y), :]
    for other in range(1, count_y):
        a_copy(other).wait_recv()
        total = total + got_a[other]
    out[0, :, GROUPS * width :] = total

    @pl.when(exists(-1, 0))
    def _():
        for other in range(count_y):
            b_copy(other).wait_recv()

    total = got_b[0]
    for other in range(1, count_y):
        total = total + got_b[other]
    out[0, :, : GROUPS * width] = total[:, : GROUPS * width]

    for slot, (step_x, step_y) in enumerate(RING):
        @pl.when(exists(-step_x, -step_y))
        def _():
            ring_copy(slot).wait_send()
    for slot, (step_x, step_y) in enumerate(HELD):
        @pl.when(exists(-step_x, -step_y))
        def _():
            halo_copy(slot).wait_send()
    for other in range(1, count_y):
        a_copy(other).wait_send()

    @pl.when(exists(1, 0))
    def _():
        for other in range(count_y):
            b_copy(other).wait_send()


def shards(counts, modes, region, stiffness, coarse_group):
    width, comps, span_x, span_y, span_z = modes.shape
    rows = GROUPS * width // counts[1]
    f32, i32 = jnp.float32, jnp.int32
    dma = pltpu.SemaphoreType.DMA
    lanes = 2 * GROUPS * width
    return pl.pallas_call(
        functools.partial(kernel, (width, span_x, span_y, span_z), counts),
        out_shape=pltpu.VMEM((1, rows, 3 * GROUPS * width), f32),
        in_specs=[
            pl.BlockSpec(memory_space=pltpu.HBM),
            pl.BlockSpec(memory_space=pltpu.HBM),
            pl.BlockSpec(memory_space=pltpu.HBM),
            pl.BlockSpec(memory_space=pltpu.HBM),
        ],
        out_specs=pl.BlockSpec(memory_space=pltpu.VMEM),
        scratch_shapes=[
            pltpu.SMEM(stiffness.shape, f32),
            pltpu.SMEM(coarse_group.shape[::-1], i32),
            pltpu.VMEM((width, comps, span_x, span_y, span_z), f32),
            pltpu.VMEM((span_x, span_y, span_z), i32),
            pltpu.VMEM((2, span_y, span_z), i32),
            pltpu.VMEM((2, span_x, span_z), i32),
            pltpu.VMEM((4, span_z), i32),
            pltpu.VMEM((span_x + 2, span_y + 8, span_z), f32),
            pltpu.VMEM((6, span_x, span_y, span_z), f32),
            pltpu.VMEM((comps, width, span_y, span_z), f32),
            pltpu.VMEM((width, comps, span_x, span_z), f32),
            pltpu.VMEM((2, comps * width, span_z), f32),
            pltpu.VMEM((GROUPS * width, lanes), f32),
            pltpu.VMEM((GROUPS * width, lanes), f32),
            pltpu.VMEM((counts[1], rows, lanes), f32),
            pltpu.VMEM((counts[1], rows, lanes), f32),
            dma((4,)),
            dma((len(RING),)), dma((len(RING),)),
            dma((len(HELD),)), dma((len(HELD),)),
            dma((counts[1],)), dma((counts[1],)),
            dma((counts[1],)), dma((counts[1],)),
        ],
        compiler_params=pltpu.CompilerParams(collective_id=0, has_side_effects=True),
    )(modes, region, stiffness, coarse_group.T)


def solution(mesh):
    counts = (mesh.shape["gx"], mesh.shape["gy"])
    in_specs = (P(None, None, "gx", "gy", None), P("gx", "gy", None), P(), P())
    out_specs = P("gx", "gy", None)
    return jax.shard_map(
        functools.partial(shards, counts), mesh=mesh, in_specs=in_specs,
        out_specs=out_specs, check_vma=False,
    )
```

```python
import functools

import jax
import jax.numpy as jnp
from jax import lax
from jax.experimental import pallas as pl
from jax.experimental.pallas import tpu as pltpu
from jax.sharding import PartitionSpec as P

GROUPS = 4

beta_shear = 0.5
mass_share = 0.1

W1, W2, W3 = 0.5, 0.25, 0.125
B1, B2, B3 = W1 * beta_shear, W2 * beta_shear / 2, W3 * beta_shear / 3
DIAG_SUM = 6 * W1 + 12 * W2 + 8 * W3 + 2 * B1 + 8 * B2 + 8 * B3

MESH = pl.DeviceIdType.MESH
RING = [(-1, -1), (-1, 0), (-1, 1), (0, -1), (0, 1), (1, -1), (1, 0), (1, 1)]
HELD = [(1, -1), (1, 1), (0, 1), (1, 0), (1, 0), (1, 0)]


def lane_steps(value):
    lane = lax.broadcasted_iota(jnp.int32, value.shape, value.ndim - 1)
    size = value.shape[-1]
    before = jnp.where(lane == 0, 0.0, pltpu.roll(value, 1, value.ndim - 1))
    after = jnp.where(lane == size - 1, 0.0, pltpu.roll(value, size - 1, value.ndim - 1))
    return before + after, after - before


def plane_parts(fields, low, high):
    span = fields[0].shape[0]

    def at(value, step):
        first, last = low + step, high + step
        start, stop = min(max(first, 0), span), min(max(last, 0), span)
        zeros = lambda n: [jnp.zeros((n,) + value.shape[1:], value.dtype)] if n else []
        if start >= stop:
            return zeros(last - first)[0]
        pieces = zeros(start - first) + [value[start:stop]] + zeros(last - stop)
        return pieces[0] if len(pieces) == 1 else jnp.concatenate(pieces, axis=0)

    def even(value):
        return at(value, -1) + at(value, 1)

    def odd(value):
        return at(value, 1) - at(value, -1)

    vx, vy, vz = fields
    (ex, ox), (ey, oy), (ez, oz) = [lane_steps(v) for v in fields]
    level = at(W1 * ex, 0) + even(W1 * vx + W2 * ex)
    share = at((W1 + B1) * vx + (W2 + B2) * ex, 0) + even((W2 + B2) * vx + (W3 + B3) * ex)
    turn = odd(B2 * vy + B3 * ey) + B2 * at(oz, 0) + B3 * even(oz)
    out_x = (level, share + turn, share - turn)
    skew = odd(oz)
    level = at(W1 * ey, 0) + even((W1 + B1) * vy + (W2 + B2) * ey) + B2 * skew
    share = at(W1 * vy + W2 * ey, 0) + even((W2 + B2) * vy + (W3 + B3) * ey) + B3 * skew
    turn = odd(B2 * vx + B3 * ex)
    out_y = (level, share + turn, share - turn)
    skew = odd(oy)
    wide = W1 * vz + (W2 + B2) * ez
    level = at((W1 + B1) * ez, 0) + even(wide) + B2 * skew
    share = at(wide, 0) + even(W2 * vz + (W3 + B3) * ez) + B3 * skew
    turn = B2 * at(ox, 0) + B3 * even(ox)
    out_z = (level, share + turn, share - turn)
    here, before, after = zip(out_x, out_y, out_z)
    return here, before, after


def stacked(value):
    high = value.astype(jnp.bfloat16)
    low = (value - high.astype(jnp.float32)).astype(jnp.bfloat16)
    cells = value.shape[0]
    join = lambda part: jnp.concatenate([part[i] for i in range(cells)], axis=1)
    return jnp.concatenate([join(high), join(low)], axis=0)


def product(left, right):
    return lax.dot_general(
        left, right, (((1,), (1,)), ((), ())), preferred_element_type=jnp.float32
    )


def folded(value, width):
    value = value[:width] + value[width:]
    return value[:, :width] + value[:, width:]


def kernel(
    shape, counts, modes, region, stiff_in, group_in, out,
    stiff, group, field, cells, ring_row, ring_side, ring_corner, sigma, diag,
    halo_x, halo_y, halo_c, part_a, part_b, got_a, got_b,
    load_sem, ring_send, ring_recv, halo_send, halo_recv, a_send, a_recv, b_send, b_recv,
):
    width, span_x, span_y, span_z = shape
    count_x, count_y = counts
    rows = GROUPS * width // count_y
    me_x, me_y = lax.axis_index("gx"), lax.axis_index("gy")

    def exists(step_x, step_y):
        ok = me_x >= 0
        if step_x < 0:
            ok = jnp.logical_and(ok, me_x > 0)
        if step_x > 0:
            ok = jnp.logical_and(ok, me_x < count_x - 1)
        if step_y < 0:
            ok = jnp.logical_and(ok, me_y > 0)
        if step_y > 0:
            ok = jnp.logical_and(ok, me_y < count_y - 1)
        return ok

    def where_is(step_x, step_y):
        return {"gx": me_x + step_x, "gy": me_y + step_y}

    load_modes = pltpu.make_async_copy(modes, field, load_sem.at[0])
    load_region = pltpu.make_async_copy(region, cells, load_sem.at[1])
    load_stiff = pltpu.make_async_copy(stiff_in, stiff, load_sem.at[2])
    load_group = pltpu.make_async_copy(group_in, group, load_sem.at[3])

    barrier = pltpu.get_barrier_semaphore()
    for step_x in (-1, 0, 1):
        @pl.when(exists(step_x, 0))
        def _():
            for other in range(1 if step_x == 0 else 0, count_y):
                there = lax.rem(me_y + other, count_y)
                pl.semaphore_signal(
                    barrier, inc=1,
                    device_id={"gx": me_x + step_x, "gy": there}, device_id_type=MESH,
                )
    load_region.start()
    load_stiff.start()
    load_group.start()
    load_modes.start()
    strips = 1 + (me_x > 0).astype(jnp.int32) + (me_x < count_x - 1).astype(jnp.int32)
    pl.semaphore_wait(barrier, strips * count_y - 1)

    def ring_refs(slot):
        step_x, step_y = RING[slot]
        edge_x = 0 if step_x > 0 else span_x - 1
        edge_y = 0 if step_y > 0 else span_y - 1
        if step_x == 0:
            return region.at[:, edge_y], ring_side.at[(step_y + 1) // 2]
        if step_y == 0:
            return region.at[edge_x], ring_row.at[(step_x + 1) // 2]
        return region.at[edge_x, edge_y], ring_corner.at[(step_x + 1) + (step_y + 1) // 2]

    def ring_copy(slot):
        step_x, step_y = RING[slot]
        source, target = ring_refs(slot)
        return pltpu.make_async_remote_copy(
            src_ref=source, dst_ref=target,
            send_sem=ring_send.at[slot], recv_sem=ring_recv.at[slot],
            device_id=where_is(-step_x, -step_y), device_id_type=MESH,
        )

    def halo_copy(slot):
        step_x, step_y = HELD[slot]
        if slot < 2:
            merged = modes.reshape(3 * width, span_x, span_y, span_z)
            source, target = merged.at[:, 0, 0 if step_y > 0 else span_y - 1], halo_c.at[slot]
        elif slot == 2:
            source, target = modes.at[:, :, :, 0], halo_y
        else:
            source, target = modes.at[:, slot - 3, 0], halo_x.at[slot - 3]
        return pltpu.make_async_remote_copy(
            src_ref=source, dst_ref=target,
            send_sem=halo_send.at[slot], recv_sem=halo_recv.at[slot],
            device_id=where_is(-step_x, -step_y), device_id_type=MESH,
        )

    for slot, (step_x, step_y) in enumerate(RING):
        @pl.when(exists(-step_x, -step_y))
        def _():
            ring_copy(slot).start()
    for slot, (step_x, step_y) in enumerate(HELD):
        @pl.when(exists(-step_x, -step_y))
        def _():
            halo_copy(slot).start()

    for slot, (step_x, step_y) in enumerate(RING):
        @pl.when(jnp.logical_not(exists(step_x, step_y)))
        def _():
            target = ring_refs(slot)[1]
            target[...] = jnp.full(target.shape, -1, jnp.int32)
    for slot, (step_x, step_y) in enumerate(HELD):
        @pl.when(jnp.logical_not(exists(step_x, step_y)))
        def _():
            target = halo_c.at[slot] if slot < 2 else halo_y if slot == 2 else halo_x.at[slot - 3]
            target[...] = jnp.zeros(target.shape, jnp.float32)

    def stiff_of(values):
        total = jnp.zeros(values.shape, jnp.float32)
        for level in range(stiff.shape[0]):
            total = jnp.where(values == level, stiff[level], total)
        return total

    load_stiff.wait()
    load_group.wait()
    load_region.wait()
    for x in range(span_x):
        sigma[1 + x, 1 : 1 + span_y] = stiff_of(cells[x])
    load_modes.wait()
    flat = field.reshape(3 * width * span_x * span_y, span_z)
    columns = 3 * span_x * span_y

    def column(comp, x, y):
        return flat[pl.ds((comp * span_x + x) * span_y + y, width, stride=columns), :]

    def plane(x):
        return [
            jnp.stack([column(comp, x, y) for y in range(span_y)]) for comp in range(3)
        ]

    for slot, (step_x, step_y) in enumerate(RING):
        @pl.when(exists(step_x, step_y))
        def _():
            ring_copy(slot).wait_recv()
    for side, x in ((0, 0), (1, span_x + 1)):
        sigma[x, 1 : 1 + span_y] = stiff_of(ring_row[side])
        sigma[x, 0:1] = stiff_of(ring_corner[2 * side : 2 * side + 1])
        sigma[x, span_y + 1 : span_y + 2] = stiff_of(ring_corner[2 * side + 1 : 2 * side + 2])
    low, high = stiff_of(ring_side[0]), stiff_of(ring_side[1])
    for x in range(span_x):
        sigma[1 + x, 0:1] = low[x : x + 1]
        sigma[1 + x, span_y + 1 : span_y + 2] = high[x : x + 1]

    def sigma_parts(x):
        level = {}
        for step in (-1, 0, 1):
            s = sigma[x, 1 + step : 1 + step + span_y]
            level[step] = (s,) + lane_steps(s)
        s0, e0, o0 = level[0]
        se, ee, oe = [level[1][i] + level[-1][i] for i in range(3)]
        so, eo, oo = [level[1][i] - level[-1][i] for i in range(3)]
        return s0, e0, o0, se, ee, oe, so, eo, oo

    parts = [sigma_parts(x) for x in range(span_x + 2)]
    for x in range(1, span_x + 1):
        s0, e0, o0, se, ee, oe, so, eo, oo = parts[x]
        fs, fe, fo, fse, fee, foe, fso, feo, foo = [
            parts[x + 1][i] + parts[x - 1][i] for i in range(9)
        ]
        ds, de, do, dse, dee, doe, dso, deo, doo = [
            parts[x + 1][i] - parts[x - 1][i] for i in range(9)
        ]
        plain = (
            (mass_share + DIAG_SUM) * s0
            + W1 * (e0 + se + fs) + W2 * (ee + fe + fse) + W3 * fee
        )
        xx = plain + B1 * fs + B2 * (fse + fe) + B3 * fee
        yy = plain + B1 * se + B2 * (fse + ee) + B3 * fee
        zz = plain + B1 * e0 + B2 * (fe + ee) + B3 * fee
        xy = B2 * dso + B3 * deo
        xz = B2 * do + B3 * doe
        yz = B2 * oo + B3 * foo
        for i, value in enumerate((xx, yy, zz, xy, xz, yz)):
            diag[i, x - 1] = 0.5 * value

    def spread(row):
        return jnp.broadcast_to(row, (width, span_z))

    def spread_sigma(x, low, high):
        return jnp.stack([spread(sigma[1 + x, 1 + y : 2 + y]) for y in range(low, high)])

    def spread_diag(i, x):
        return jnp.stack([spread(diag[i, x, y : y + 1]) for y in range(span_y)])

    own = jnp.zeros((2 * width, 2 * width), jnp.float32)
    here, before, after, fields, weights = [], [], [], [], []
    edge_here, edge_before, edge_after = [], [], []
    for x in range(span_x):
        last = x == span_x - 1
        v = plane(x)
        s = spread_sigma(x, 0, span_y)
        a, b, c = plane_parts(v, -1 if last else 0, span_y + 1)
        if last:
            beyond = c
            a, b = [[t[1:] for t in group_] for group_ in (a, b)]
            sv = [s * t for t in v]
            ea, eb, ec = plane_parts(sv, -1, span_y + 1)
            beyond_s = ec
            ea, eb = [[t[span_y + 1 :] for t in group_] for group_ in (ea, eb)]
        else:
            sv = [s[span_y - 1 :] * t[span_y - 1 :] for t in v]
            ea, eb, ec = plane_parts(sv, 1, 2)
        here.append(a); before.append(b); after.append(c)
        edge_here.append(ea); edge_before.append(eb); edge_after.append(ec)
        fields.append(v); weights.append(s)

    side = []
    for x in range(span_x):
        reach = list(here[x])
        edge = list(edge_here[x])
        if x + 1 < span_x:
            reach = [r + t for r, t in zip(reach, before[x + 1])]
            edge = [r + t for r, t in zip(edge, edge_before[x + 1])]
        if x > 0:
            reach = [r + t for r, t in zip(reach, after[x - 1])]
            edge = [r + t for r, t in zip(edge, edge_after[x - 1])]
        v, s = fields[x], weights[x]
        dxx, dyy, dzz, dxy, dxz, dyz = [spread_diag(i, x) for i in range(6)]
        applied = [
            dxx * v[0] + dxy * v[1] + dxz * v[2],
            dxy * v[0] + dyy * v[1] + dyz * v[2],
            dxz * v[0] + dyz * v[1] + dzz * v[2],
        ]
        for comp in range(3):
            left = applied[comp] - s * reach[comp][:span_y]
            own = own + product(stacked(left), stacked(v[comp]))
        s_side = spread_sigma(x, span_y, span_y + 1)
        side.append([stacked(s_side * reach[i][span_y:] + edge[i]) for i in range(3)])
    s_row = spread_sigma(span_x, -1, span_y + 1)
    row = [s_row * beyond[i] + beyond_s[i] for i in range(3)]
    row_mid = [stacked(t[1 : span_y + 1]) for t in row]
    row_low = [stacked(t[:1]) for t in row]
    row_high = [stacked(t[span_y + 1 :]) for t in row]
    block = folded(own, width)
    block = block + block.T

    def arrived(slot):
        @pl.when(exists(*HELD[slot]))
        def _():
            halo_copy(slot).wait_recv()

    def pair(left, right):
        total = product(left[0], right[0])
        for l, r in zip(left[1:], right[1:]):
            total = total + product(l, r)
        return total

    def corner(i):
        return [stacked(halo_c[i, pl.ds(comp, width, stride=3), :][None]) for comp in range(3)]

    arrived(2)
    flat_y = halo_y.reshape(3 * width * span_x, span_z)
    c_side = -folded(pair(
        [side[x][comp] for x in range(span_x) for comp in range(3)],
        [
            stacked(flat_y[pl.ds(comp * span_x + x, width, stride=3 * span_x), :][None])
            for x in range(span_x) for comp in range(3)
        ],
    ), width)
    arrived(0)
    c_low = -folded(pair(row_low, corner(0)), width)
    arrived(1)
    c_high = -folded(pair(row_high, corner(1)), width)
    next_x = jnp.minimum(me_x + 1, count_x - 1)
    next_y = jnp.minimum(me_y + 1, count_y - 1)
    last_y = jnp.maximum(me_y - 1, 0)
    g_self, g_side = group[me_y, me_x], group[next_y, me_x]
    g_low, g_mid, g_high = group[last_y, next_x], group[me_y, next_x], group[next_y, next_x]
    slot_of = lax.broadcasted_iota(jnp.int32, (width, GROUPS * width), 1) // width

    def placed(value, label):
        return jnp.where(slot_of == label, jnp.concatenate([value] * GROUPS, axis=1), 0.0)

    level = placed(block, g_self) + placed(c_side, g_side)
    ahead = placed(c_low, g_low) + placed(c_high, g_high)
    none = jnp.zeros_like(level)
    back_side = jnp.concatenate([placed(c_side.T, g_self), none], axis=1)
    back_low, back_high = placed(c_low.T, g_self), placed(c_high.T, g_self)
    backs = [
        jnp.where(g_low == g, back_low, 0.0) + jnp.where(g_high == g, back_high, 0.0)
        for g in range(GROUPS)
    ]

    @pl.when(jnp.logical_not(exists(-1, 0)))
    def _():
        got_b[...] = jnp.zeros(got_b.shape, jnp.float32)

    def rows_of(there):
        return pl.ds(pl.multiple_of(there * rows, rows), rows)

    def a_copy(other):
        there = lax.rem(me_y + other, count_y)
        return pltpu.make_async_remote_copy(
            src_ref=part_a.at[rows_of(there)], dst_ref=got_a.at[other],
            send_sem=a_send.at[other], recv_sem=a_recv.at[other],
            device_id={"gx": me_x, "gy": there}, device_id_type=MESH,
        )

    def b_copy(other):
        there = lax.rem(me_y + other, count_y)
        return pltpu.make_async_remote_copy(
            src_ref=part_b.at[there], dst_ref=got_b.at[other],
            send_sem=b_send.at[other], recv_sem=b_recv.at[other],
            device_id={"gx": me_x + 1, "gy": there}, device_id_type=MESH,
        )

    c_mid = jnp.zeros((2 * width, 2 * width), jnp.float32)
    for comp in range(3):
        arrived(3 + comp)
        flat_x = halo_x.at[comp].reshape(width * span_y, span_z)
        near = jnp.stack([flat_x[pl.ds(y, width, stride=span_y), :] for y in range(span_y)])
        c_mid = c_mid + product(row_mid[comp], stacked(near))
    c_mid = -folded(c_mid, width)

    back_mid = placed(c_mid.T, g_self)
    back = jnp.concatenate(
        [backs[g] + jnp.where(g_mid == g, back_mid, 0.0) for g in range(GROUPS)], axis=0
    )
    half = rows // 2
    for there in range(count_y):
        start = there * rows
        part_b[there] = jnp.concatenate(
            [back[start : start + half], back[start + half : start + rows]], axis=1
        )

    @pl.when(exists(1, 0))
    def _():
        for other in range(count_y):
            b_copy(other).start()

    strip = jnp.concatenate([level, ahead + placed(c_mid, g_mid)], axis=1)
    for g in range(GROUPS):
        part_a[g * width : (g + 1) * width] = (
            jnp.where(g_self == g, strip, 0.0) + jnp.where(g_side == g, back_side, 0.0)
        )

    for other in range(1, count_y):
        a_copy(other).start()

    total = part_a[rows_of(me_y), :]
    for other in range(1, count_y):
        a_copy(other).wait_recv()
        total = total + got_a[other]
    out[0, :, GROUPS * width :] = total

    @pl.when(exists(-1, 0))
    def _():
        for other in range(count_y):
            b_copy(other).wait_recv()

    total = got_b[0]
    for other in range(1, count_y):
        total = total + got_b[other]
    out[0, :half, : GROUPS * width] = total[:, : GROUPS * width]
    out[0, half:, : GROUPS * width] = total[:, GROUPS * width :]

    for slot, (step_x, step_y) in enumerate(RING):
        @pl.when(exists(-step_x, -step_y))
        def _():
            ring_copy(slot).wait_send()
    for slot, (step_x, step_y) in enumerate(HELD):
        @pl.when(exists(-step_x, -step_y))
        def _():
            halo_copy(slot).wait_send()
    for other in range(1, count_y):
        a_copy(other).wait_send()

    @pl.when(exists(1, 0))
    def _():
        for other in range(count_y):
            b_copy(other).wait_send()


def shards(counts, modes, region, stiffness, coarse_group):
    width, comps, span_x, span_y, span_z = modes.shape
    rows = GROUPS * width // counts[1]
    f32, i32 = jnp.float32, jnp.int32
    dma = pltpu.SemaphoreType.DMA
    lanes = 2 * GROUPS * width
    return pl.pallas_call(
        functools.partial(kernel, (width, span_x, span_y, span_z), counts),
        out_shape=pltpu.VMEM((1, rows, 3 * GROUPS * width), f32),
        in_specs=[
            pl.BlockSpec(memory_space=pltpu.HBM),
            pl.BlockSpec(memory_space=pltpu.HBM),
            pl.BlockSpec(memory_space=pltpu.HBM),
            pl.BlockSpec(memory_space=pltpu.HBM),
        ],
        out_specs=pl.BlockSpec(memory_space=pltpu.VMEM),
        scratch_shapes=[
            pltpu.SMEM(stiffness.shape, f32),
            pltpu.SMEM(coarse_group.shape[::-1], i32),
            pltpu.VMEM((width, comps, span_x, span_y, span_z), f32),
            pltpu.VMEM((span_x, span_y, span_z), i32),
            pltpu.VMEM((2, span_y, span_z), i32),
            pltpu.VMEM((2, span_x, span_z), i32),
            pltpu.VMEM((4, span_z), i32),
            pltpu.VMEM((span_x + 2, span_y + 8, span_z), f32),
            pltpu.VMEM((6, span_x, span_y, span_z), f32),
            pltpu.VMEM((comps, width, span_y, span_z), f32),
            pltpu.VMEM((width, comps, span_x, span_z), f32),
            pltpu.VMEM((2, comps * width, span_z), f32),
            pltpu.VMEM((GROUPS * width, lanes), f32),
            pltpu.VMEM((counts[1], rows // 2, lanes), f32),
            pltpu.VMEM((counts[1], rows, lanes), f32),
            pltpu.VMEM((counts[1], rows // 2, lanes), f32),
            dma((4,)),
            dma((len(RING),)), dma((len(RING),)),
            dma((len(HELD),)), dma((len(HELD),)),
            dma((counts[1],)), dma((counts[1],)),
            dma((counts[1],)), dma((counts[1],)),
        ],
        compiler_params=pltpu.CompilerParams(collective_id=0, has_side_effects=True),
    )(modes, region, stiffness, coarse_group.T)


def solution(mesh):
    counts = (mesh.shape["gx"], mesh.shape["gy"])
    in_specs = (P(None, None, "gx", "gy", None), P("gx", "gy", None), P(), P())
    out_specs = P("gx", "gy", None)
    return jax.shard_map(
        functools.partial(shards, counts), mesh=mesh, in_specs=in_specs,
        out_specs=out_specs, check_vma=False,
    )
```

```python
import functools

import jax
import jax.numpy as jnp
from jax import lax
from jax.experimental import pallas as pl
from jax.experimental.pallas import tpu as pltpu
from jax.sharding import PartitionSpec as P

GROUPS = 4

beta_shear = 0.5
mass_share = 0.1

W1, W2, W3 = 0.5, 0.25, 0.125
B1, B2, B3 = W1 * beta_shear, W2 * beta_shear / 2, W3 * beta_shear / 3
DIAG_SUM = 6 * W1 + 12 * W2 + 8 * W3 + 2 * B1 + 8 * B2 + 8 * B3

MESH = pl.DeviceIdType.MESH
RING = [(-1, -1), (-1, 0), (-1, 1), (0, -1), (0, 1), (1, -1), (1, 0), (1, 1)]
HELD = [(1, -1), (1, 1), (0, 1), (1, 0), (1, 0), (1, 0)]


def lane_steps(value):
    lane = lax.broadcasted_iota(jnp.int32, value.shape, value.ndim - 1)
    size = value.shape[-1]
    before = jnp.where(lane == 0, 0.0, pltpu.roll(value, 1, value.ndim - 1))
    after = jnp.where(lane == size - 1, 0.0, pltpu.roll(value, size - 1, value.ndim - 1))
    return before + after, after - before


def plane_parts(fields, low, high):
    span = fields[0].shape[0]

    def at(value, step):
        first, last = low + step, high + step
        start, stop = min(max(first, 0), span), min(max(last, 0), span)
        zeros = lambda n: [jnp.zeros((n,) + value.shape[1:], value.dtype)] if n else []
        if start >= stop:
            return zeros(last - first)[0]
        pieces = zeros(start - first) + [value[start:stop]] + zeros(last - stop)
        return pieces[0] if len(pieces) == 1 else jnp.concatenate(pieces, axis=0)

    def even(value):
        return at(value, -1) + at(value, 1)

    def odd(value):
        return at(value, 1) - at(value, -1)

    vx, vy, vz = fields
    (ex, ox), (ey, oy), (ez, oz) = [lane_steps(v) for v in fields]
    level = at(W1 * ex, 0) + even(W1 * vx + W2 * ex)
    share = at((W1 + B1) * vx + (W2 + B2) * ex, 0) + even((W2 + B2) * vx + (W3 + B3) * ex)
    turn = odd(B2 * vy + B3 * ey) + B2 * at(oz, 0) + B3 * even(oz)
    out_x = (level, share + turn, share - turn)
    skew = odd(oz)
    level = at(W1 * ey, 0) + even((W1 + B1) * vy + (W2 + B2) * ey) + B2 * skew
    share = at(W1 * vy + W2 * ey, 0) + even((W2 + B2) * vy + (W3 + B3) * ey) + B3 * skew
    turn = odd(B2 * vx + B3 * ex)
    out_y = (level, share + turn, share - turn)
    skew = odd(oy)
    wide = W1 * vz + (W2 + B2) * ez
    level = at((W1 + B1) * ez, 0) + even(wide) + B2 * skew
    share = at(wide, 0) + even(W2 * vz + (W3 + B3) * ez) + B3 * skew
    turn = B2 * at(ox, 0) + B3 * even(ox)
    out_z = (level, share + turn, share - turn)
    here, before, after = zip(out_x, out_y, out_z)
    return here, before, after


def stacked(value):
    high = value.astype(jnp.bfloat16)
    low = (value - high.astype(jnp.float32)).astype(jnp.bfloat16)
    cells = value.shape[0]
    join = lambda part: jnp.concatenate([part[i] for i in range(cells)], axis=1)
    return jnp.concatenate([join(high), join(low)], axis=0)


def product(left, right):
    return lax.dot_general(
        left, right, (((1,), (1,)), ((), ())), preferred_element_type=jnp.float32
    )


def folded(value, width):
    value = value[:width] + value[width:]
    return value[:, :width] + value[:, width:]


def kernel(
    shape, counts, modes, region, stiff_in, group_in, out,
    stiff, group, field, cells, ring_row, ring_side, ring_corner, sigma, diag,
    halo_x, halo_y, halo_c, part_a, part_b, got_a, got_b,
    load_sem, ring_send, ring_recv, halo_send, halo_recv, a_send, a_recv, b_send, b_recv,
):
    width, span_x, span_y, span_z = shape
    count_x, count_y = counts
    rows = GROUPS * width // count_y
    me_x, me_y = lax.axis_index("gx"), lax.axis_index("gy")

    def exists(step_x, step_y):
        ok = me_x >= 0
        if step_x < 0:
            ok = jnp.logical_and(ok, me_x > 0)
        if step_x > 0:
            ok = jnp.logical_and(ok, me_x < count_x - 1)
        if step_y < 0:
            ok = jnp.logical_and(ok, me_y > 0)
        if step_y > 0:
            ok = jnp.logical_and(ok, me_y < count_y - 1)
        return ok

    def where_is(step_x, step_y):
        return {"gx": me_x + step_x, "gy": me_y + step_y}

    load_modes = pltpu.make_async_copy(modes, field, load_sem.at[0])
    load_region = pltpu.make_async_copy(region, cells, load_sem.at[1])
    load_stiff = pltpu.make_async_copy(stiff_in, stiff, load_sem.at[2])
    load_group = pltpu.make_async_copy(group_in, group, load_sem.at[3])

    barrier = pltpu.get_barrier_semaphore()
    for step_x in (-1, 0, 1):
        @pl.when(exists(step_x, 0))
        def _():
            for other in range(1 if step_x == 0 else 0, count_y):
                there = lax.rem(me_y + other, count_y)
                pl.semaphore_signal(
                    barrier, inc=1,
                    device_id={"gx": me_x + step_x, "gy": there}, device_id_type=MESH,
                )
    load_region.start()
    load_stiff.start()
    load_group.start()
    load_modes.start()
    strips = 1 + (me_x > 0).astype(jnp.int32) + (me_x < count_x - 1).astype(jnp.int32)
    pl.semaphore_wait(barrier, strips * count_y - 1)

    def ring_refs(slot):
        step_x, step_y = RING[slot]
        edge_x = 0 if step_x > 0 else span_x - 1
        edge_y = 0 if step_y > 0 else span_y - 1
        if step_x == 0:
            return cells.at[:, edge_y], ring_side.at[(step_y + 1) // 2]
        if step_y == 0:
            return cells.at[edge_x], ring_row.at[(step_x + 1) // 2]
        return cells.at[edge_x, edge_y], ring_corner.at[(step_x + 1) + (step_y + 1) // 2]

    def ring_copy(slot):
        step_x, step_y = RING[slot]
        source, target = ring_refs(slot)
        return pltpu.make_async_remote_copy(
            src_ref=source, dst_ref=target,
            send_sem=ring_send.at[slot], recv_sem=ring_recv.at[slot],
            device_id=where_is(-step_x, -step_y), device_id_type=MESH,
        )

    def halo_copy(slot):
        step_x, step_y = HELD[slot]
        if slot < 2:
            merged = field.reshape(3 * width, span_x, span_y, span_z)
            source, target = merged.at[:, 0, 0 if step_y > 0 else span_y - 1], halo_c.at[slot]
        elif slot == 2:
            source, target = field.at[:, :, :, 0], halo_y
        else:
            source, target = field.at[:, slot - 3, 0], halo_x.at[slot - 3]
        return pltpu.make_async_remote_copy(
            src_ref=source, dst_ref=target,
            send_sem=halo_send.at[slot], recv_sem=halo_recv.at[slot],
            device_id=where_is(-step_x, -step_y), device_id_type=MESH,
        )

    load_region.wait()
    for slot, (step_x, step_y) in enumerate(RING):
        @pl.when(exists(-step_x, -step_y))
        def _():
            ring_copy(slot).start()
    load_modes.wait()
    for slot, (step_x, step_y) in enumerate(HELD):
        @pl.when(exists(-step_x, -step_y))
        def _():
            halo_copy(slot).start()

    for slot, (step_x, step_y) in enumerate(RING):
        @pl.when(jnp.logical_not(exists(step_x, step_y)))
        def _():
            target = ring_refs(slot)[1]
            target[...] = jnp.full(target.shape, -1, jnp.int32)
    for slot, (step_x, step_y) in enumerate(HELD):
        @pl.when(jnp.logical_not(exists(step_x, step_y)))
        def _():
            target = halo_c.at[slot] if slot < 2 else halo_y if slot == 2 else halo_x.at[slot - 3]
            target[...] = jnp.zeros(target.shape, jnp.float32)

    def stiff_of(values):
        total = jnp.zeros(values.shape, jnp.float32)
        for level in range(stiff.shape[0]):
            total = jnp.where(values == level, stiff[level], total)
        return total

    load_stiff.wait()
    load_group.wait()
    for x in range(span_x):
        sigma[1 + x, 1 : 1 + span_y] = stiff_of(cells[x])
    flat = field.reshape(3 * width * span_x * span_y, span_z)
    columns = 3 * span_x * span_y

    def column(comp, x, y):
        return flat[pl.ds((comp * span_x + x) * span_y + y, width, stride=columns), :]

    def plane(x):
        return [
            jnp.stack([column(comp, x, y) for y in range(span_y)]) for comp in range(3)
        ]

    for slot, (step_x, step_y) in enumerate(RING):
        @pl.when(exists(step_x, step_y))
        def _():
            ring_copy(slot).wait_recv()
    for side, x in ((0, 0), (1, span_x + 1)):
        sigma[x, 1 : 1 + span_y] = stiff_of(ring_row[side])
        sigma[x, 0:1] = stiff_of(ring_corner[2 * side : 2 * side + 1])
        sigma[x, span_y + 1 : span_y + 2] = stiff_of(ring_corner[2 * side + 1 : 2 * side + 2])
    low, high = stiff_of(ring_side[0]), stiff_of(ring_side[1])
    for x in range(span_x):
        sigma[1 + x, 0:1] = low[x : x + 1]
        sigma[1 + x, span_y + 1 : span_y + 2] = high[x : x + 1]

    def sigma_parts(x):
        level = {}
        for step in (-1, 0, 1):
            s = sigma[x, 1 + step : 1 + step + span_y]
            level[step] = (s,) + lane_steps(s)
        s0, e0, o0 = level[0]
        se, ee, oe = [level[1][i] + level[-1][i] for i in range(3)]
        so, eo, oo = [level[1][i] - level[-1][i] for i in range(3)]
        return s0, e0, o0, se, ee, oe, so, eo, oo

    parts = [sigma_parts(x) for x in range(span_x + 2)]
    for x in range(1, span_x + 1):
        s0, e0, o0, se, ee, oe, so, eo, oo = parts[x]
        fs, fe, fo, fse, fee, foe, fso, feo, foo = [
            parts[x + 1][i] + parts[x - 1][i] for i in range(9)
        ]
        ds, de, do, dse, dee, doe, dso, deo, doo = [
            parts[x + 1][i] - parts[x - 1][i] for i in range(9)
        ]
        plain = (
            (mass_share + DIAG_SUM) * s0
            + W1 * (e0 + se + fs) + W2 * (ee + fe + fse) + W3 * fee
        )
        xx = plain + B1 * fs + B2 * (fse + fe) + B3 * fee
        yy = plain + B1 * se + B2 * (fse + ee) + B3 * fee
        zz = plain + B1 * e0 + B2 * (fe + ee) + B3 * fee
        xy = B2 * dso + B3 * deo
        xz = B2 * do + B3 * doe
        yz = B2 * oo + B3 * foo
        for i, value in enumerate((xx, yy, zz, xy, xz, yz)):
            diag[i, x - 1] = 0.5 * value

    def spread(row):
        return jnp.broadcast_to(row, (width, span_z))

    def spread_sigma(x, low, high):
        return jnp.stack([spread(sigma[1 + x, 1 + y : 2 + y]) for y in range(low, high)])

    def spread_diag(i, x):
        return jnp.stack([spread(diag[i, x, y : y + 1]) for y in range(span_y)])

    own = jnp.zeros((2 * width, 2 * width), jnp.float32)
    here, before, after, fields, weights = [], [], [], [], []
    edge_here, edge_before, edge_after = [], [], []
    for x in range(span_x):
        last = x == span_x - 1
        v = plane(x)
        s = spread_sigma(x, 0, span_y)
        a, b, c = plane_parts(v, -1 if last else 0, span_y + 1)
        if last:
            beyond = c
            a, b = [[t[1:] for t in group_] for group_ in (a, b)]
            sv = [s * t for t in v]
            ea, eb, ec = plane_parts(sv, -1, span_y + 1)
            beyond_s = ec
            ea, eb = [[t[span_y + 1 :] for t in group_] for group_ in (ea, eb)]
        else:
            sv = [s[span_y - 1 :] * t[span_y - 1 :] for t in v]
            ea, eb, ec = plane_parts(sv, 1, 2)
        here.append(a); before.append(b); after.append(c)
        edge_here.append(ea); edge_before.append(eb); edge_after.append(ec)
        fields.append(v); weights.append(s)

    side = []
    for x in range(span_x):
        reach = list(here[x])
        edge = list(edge_here[x])
        if x + 1 < span_x:
            reach = [r + t for r, t in zip(reach, before[x + 1])]
            edge = [r + t for r, t in zip(edge, edge_before[x + 1])]
        if x > 0:
            reach = [r + t for r, t in zip(reach, after[x - 1])]
            edge = [r + t for r, t in zip(edge, edge_after[x - 1])]
        v, s = fields[x], weights[x]
        dxx, dyy, dzz, dxy, dxz, dyz = [spread_diag(i, x) for i in range(6)]
        applied = [
            dxx * v[0] + dxy * v[1] + dxz * v[2],
            dxy * v[0] + dyy * v[1] + dyz * v[2],
            dxz * v[0] + dyz * v[1] + dzz * v[2],
        ]
        for comp in range(3):
            left = applied[comp] - s * reach[comp][:span_y]
            own = own + product(stacked(left), stacked(v[comp]))
        s_side = spread_sigma(x, span_y, span_y + 1)
        side.append([stacked(s_side * reach[i][span_y:] + edge[i]) for i in range(3)])
    s_row = spread_sigma(span_x, -1, span_y + 1)
    row = [s_row * beyond[i] + beyond_s[i] for i in range(3)]
    row_mid = [stacked(t[1 : span_y + 1]) for t in row]
    row_low = [stacked(t[:1]) for t in row]
    row_high = [stacked(t[span_y + 1 :]) for t in row]
    block = folded(own, width)
    block = block + block.T

    def arrived(slot):
        @pl.when(exists(*HELD[slot]))
        def _():
            halo_copy(slot).wait_recv()

    def pair(left, right):
        total = product(left[0], right[0])
        for l, r in zip(left[1:], right[1:]):
            total = total + product(l, r)
        return total

    def corner(i):
        return [stacked(halo_c[i, pl.ds(comp, width, stride=3), :][None]) for comp in range(3)]

    arrived(2)
    flat_y = halo_y.reshape(3 * width * span_x, span_z)
    c_side = -folded(pair(
        [side[x][comp] for x in range(span_x) for comp in range(3)],
        [
            stacked(flat_y[pl.ds(comp * span_x + x, width, stride=3 * span_x), :][None])
            for x in range(span_x) for comp in range(3)
        ],
    ), width)
    arrived(0)
    c_low = -folded(pair(row_low, corner(0)), width)
    arrived(1)
    c_high = -folded(pair(row_high, corner(1)), width)
    next_x = jnp.minimum(me_x + 1, count_x - 1)
    next_y = jnp.minimum(me_y + 1, count_y - 1)
    last_y = jnp.maximum(me_y - 1, 0)
    g_self, g_side = group[me_y, me_x], group[next_y, me_x]
    g_low, g_mid, g_high = group[last_y, next_x], group[me_y, next_x], group[next_y, next_x]
    slot_of = lax.broadcasted_iota(jnp.int32, (width, GROUPS * width), 1) // width

    def placed(value, label):
        return jnp.where(slot_of == label, jnp.concatenate([value] * GROUPS, axis=1), 0.0)

    level = placed(block, g_self) + placed(c_side, g_side)
    ahead = placed(c_low, g_low) + placed(c_high, g_high)
    none = jnp.zeros_like(level)
    back_side = jnp.concatenate([placed(c_side.T, g_self), none], axis=1)
    back_low, back_high = placed(c_low.T, g_self), placed(c_high.T, g_self)
    backs = [
        jnp.where(g_low == g, back_low, 0.0) + jnp.where(g_high == g, back_high, 0.0)
        for g in range(GROUPS)
    ]

    @pl.when(jnp.logical_not(exists(-1, 0)))
    def _():
        got_b[...] = jnp.zeros(got_b.shape, jnp.float32)

    def rows_of(there):
        return pl.ds(pl.multiple_of(there * rows, rows), rows)

    def a_copy(other):
        there = lax.rem(me_y + other, count_y)
        return pltpu.make_async_remote_copy(
            src_ref=part_a.at[rows_of(there)], dst_ref=got_a.at[other],
            send_sem=a_send.at[other], recv_sem=a_recv.at[other],
            device_id={"gx": me_x, "gy": there}, device_id_type=MESH,
        )

    def b_copy(other):
        there = lax.rem(me_y + other, count_y)
        return pltpu.make_async_remote_copy(
            src_ref=part_b.at[there], dst_ref=got_b.at[other],
            send_sem=b_send.at[other], recv_sem=b_recv.at[other],
            device_id={"gx": me_x + 1, "gy": there}, device_id_type=MESH,
        )

    c_mid = jnp.zeros((2 * width, 2 * width), jnp.float32)
    for comp in range(3):
        arrived(3 + comp)
        flat_x = halo_x.at[comp].reshape(width * span_y, span_z)
        near = jnp.stack([flat_x[pl.ds(y, width, stride=span_y), :] for y in range(span_y)])
        c_mid = c_mid + product(row_mid[comp], stacked(near))
    c_mid = -folded(c_mid, width)

    back_mid = placed(c_mid.T, g_self)
    back = jnp.concatenate(
        [backs[g] + jnp.where(g_mid == g, back_mid, 0.0) for g in range(GROUPS)], axis=0
    )
    half = rows // 2
    for there in range(count_y):
        start = there * rows
        part_b[there] = jnp.concatenate(
            [back[start : start + half], back[start + half : start + rows]], axis=1
        )

    @pl.when(exists(1, 0))
    def _():
        for other in range(count_y):
            b_copy(other).start()

    strip = jnp.concatenate([level, ahead + placed(c_mid, g_mid)], axis=1)
    for g in range(GROUPS):
        part_a[g * width : (g + 1) * width] = (
            jnp.where(g_self == g, strip, 0.0) + jnp.where(g_side == g, back_side, 0.0)
        )

    for other in range(1, count_y):
        a_copy(other).start()

    total = part_a[rows_of(me_y), :]
    for other in range(1, count_y):
        a_copy(other).wait_recv()
        total = total + got_a[other]
    out[0, :, GROUPS * width :] = total

    @pl.when(exists(-1, 0))
    def _():
        for other in range(count_y):
            b_copy(other).wait_recv()

    total = got_b[0]
    for other in range(1, count_y):
        total = total + got_b[other]
    out[0, :half, : GROUPS * width] = total[:, : GROUPS * width]
    out[0, half:, : GROUPS * width] = total[:, GROUPS * width :]

    for slot, (step_x, step_y) in enumerate(RING):
        @pl.when(exists(-step_x, -step_y))
        def _():
            ring_copy(slot).wait_send()
    for slot, (step_x, step_y) in enumerate(HELD):
        @pl.when(exists(-step_x, -step_y))
        def _():
            halo_copy(slot).wait_send()
    for other in range(1, count_y):
        a_copy(other).wait_send()

    @pl.when(exists(1, 0))
    def _():
        for other in range(count_y):
            b_copy(other).wait_send()


def shards(counts, modes, region, stiffness, coarse_group):
    width, comps, span_x, span_y, span_z = modes.shape
    rows = GROUPS * width // counts[1]
    f32, i32 = jnp.float32, jnp.int32
    dma = pltpu.SemaphoreType.DMA
    lanes = 2 * GROUPS * width
    return pl.pallas_call(
        functools.partial(kernel, (width, span_x, span_y, span_z), counts),
        out_shape=pltpu.VMEM((1, rows, 3 * GROUPS * width), f32),
        in_specs=[
            pl.BlockSpec(memory_space=pltpu.HBM),
            pl.BlockSpec(memory_space=pltpu.HBM),
            pl.BlockSpec(memory_space=pltpu.HBM),
            pl.BlockSpec(memory_space=pltpu.HBM),
        ],
        out_specs=pl.BlockSpec(memory_space=pltpu.VMEM),
        scratch_shapes=[
            pltpu.SMEM(stiffness.shape, f32),
            pltpu.SMEM(coarse_group.shape[::-1], i32),
            pltpu.VMEM((width, comps, span_x, span_y, span_z), f32),
            pltpu.VMEM((span_x, span_y, span_z), i32),
            pltpu.VMEM((2, span_y, span_z), i32),
            pltpu.VMEM((2, span_x, span_z), i32),
            pltpu.VMEM((4, span_z), i32),
            pltpu.VMEM((span_x + 2, span_y + 8, span_z), f32),
            pltpu.VMEM((6, span_x, span_y, span_z), f32),
            pltpu.VMEM((comps, width, span_y, span_z), f32),
            pltpu.VMEM((width, comps, span_x, span_z), f32),
            pltpu.VMEM((2, comps * width, span_z), f32),
            pltpu.VMEM((GROUPS * width, lanes), f32),
            pltpu.VMEM((counts[1], rows // 2, lanes), f32),
            pltpu.VMEM((counts[1], rows, lanes), f32),
            pltpu.VMEM((counts[1], rows // 2, lanes), f32),
            dma((4,)),
            dma((len(RING),)), dma((len(RING),)),
            dma((len(HELD),)), dma((len(HELD),)),
            dma((counts[1],)), dma((counts[1],)),
            dma((counts[1],)), dma((counts[1],)),
        ],
        compiler_params=pltpu.CompilerParams(collective_id=0, has_side_effects=True),
    )(modes, region, stiffness, coarse_group.T)


def solution(mesh):
    counts = (mesh.shape["gx"], mesh.shape["gy"])
    in_specs = (P(None, None, "gx", "gy", None), P("gx", "gy", None), P(), P())
    out_specs = P("gx", "gy", None)
    return jax.shard_map(
        functools.partial(shards, counts), mesh=mesh, in_specs=in_specs,
        out_specs=out_specs, check_vma=False,
    )
```
